32 devices in a mesh: slab: 16 (over z, y, x), sub: 2 (over core).
Axes of the slice: x: 2, y: 2, z: 4, core: 2. Of those that a mesh axis runs over, the one named last changes fastest.
Arguments:
- start: float32 [4, 96, 32, 256], P(None, 'slab', 'sub'), may hold values from -6 to 6
- wind: float32 [3, 96, 32, 256], P(None, 'slab', 'sub'), may hold values from -4 to 4
- reaction: float32 [96, 32, 256], P('slab', 'sub'), may hold values from 0.5 to 4
- mass: float32 [96, 32, 256], P('slab', 'sub'), may hold values from 0.5 to 2
Outputs:
- basis: float32 [4, 4, 96, 32, 256], P(None, None, 'slab', 'sub')
- search: float32 [3, 4, 96, 32, 256], P(None, None, 'slab', 'sub')
- hessenberg: float32 [4, 3], replicated
The draws below stay inside these ranges and needn't reach their ends.
All inputs are finite; a program needn't handle non-finite values.
Results may differ from the reference program's by a relative error of at most 0.0003.
Values sent between devices are 32-bit elements; how exact they have to be, the bound alone decides.
No kernel may reach another device: no remote copies, remote signals or barrier semaphores. Data moves between devices by JAX's collectives and lax.ppermute only.
A program may use at most 64 MiB of HBM per device.

```python
import math
import jax
import jax.numpy as jnp

NZ = 256
ITERS = 3
NX = 96
NY = 32


def level_of(key, shape, split, low, top_value):
    loudness, own = 1.0, jax.random.fold_in(key, 6)
    for axis_at, blocks in split:
        draws = jnp.exp(jax.random.uniform(jax.random.fold_in(own, axis_at), (blocks,), jnp.float32, low / len(split), top_value / len(split)))
        loudness = loudness * jnp.repeat(draws, shape[axis_at] // blocks).reshape([-1 if axis == axis_at else 1 for axis in range(len(shape))])
    return loudness


def normal_values(own_key, shape, spread, reach, split=(), held_as=jnp.bfloat16):
    loudness = level_of(own_key, shape, split, -0.22, 0.18) if split else 1.0
    values = jax.random.normal(own_key, shape, jnp.float32) * spread * loudness
    return jnp.minimum(jnp.maximum(values, -reach), reach).astype(held_as)


def setup_inputs(seed: int = 0) -> dict:
    splits = jax.random.split(jax.random.key(seed), 5)
    return {
        "start": normal_values(splits[0], (4, NX, NY, NZ), 1.0, 6.0, ((1, 16), (2, 2)), jnp.float32),
        "wind": normal_values(splits[1], (3, NX, NY, NZ), 1.0, 4.0, ((1, 16), (2, 2)), jnp.float32),
        "reaction": jnp.clip(jnp.exp(math.log(4.0) - 2.0794415 * jax.random.uniform(splits[2], (NX, NY, NZ), jnp.float32) ** level_of(splits[2], (NX, NY, NZ), ((0, 16), (1, 2)), -0.2, 0.2)), 0.5, 4.0),
        "mass": jnp.clip(jnp.exp(math.log(2.0) - 1.3862944 * jax.random.uniform(splits[3], (NX, NY, NZ), jnp.float32) ** level_of(splits[3], (NX, NY, NZ), ((0, 16), (1, 2)), -0.2, 0.2)), 0.5, 2.0),
    }


def grid_pad(field):
    return jnp.pad(field, [(0, 0)] * (field.ndim - 3) + [(1, 1), (1, 1), (0, 0)])

def neighbour_sets(padded):
    center = padded[..., 1:-1, 1:-1, :]
    zero_face = jnp.zeros_like(center[..., :1])
    plus_side = (padded[..., 2:, 1:-1, :], padded[..., 1:-1, 2:, :], jnp.concatenate([center[..., 1:], zero_face], -1))
    minus_side = (padded[..., :-2, 1:-1, :], padded[..., 1:-1, :-2, :], jnp.concatenate([zero_face, center[..., :-1]], -1))
    return (center, plus_side, minus_side)

def six_sum(plus_side, minus_side):
    total = plus_side[0] + minus_side[0]
    total = total + plus_side[1] + minus_side[1]
    return total + plus_side[2] + minus_side[2]

def transport(padded, reaction_k, wind_k):
    center, plus_side, minus_side = neighbour_sets(padded)
    convect = wind_k[0] * (plus_side[0] - minus_side[0])
    convect = convect + wind_k[1] * (plus_side[1] - minus_side[1])
    convect = convect + wind_k[2] * (plus_side[2] - minus_side[2])
    return (6.0 + reaction_k) * center - six_sum(plus_side, minus_side) + 0.5 * convect

def gradient(padded):
    center, plus_side, minus_side = neighbour_sets(padded)
    return jnp.stack([0.5 * (plus_side[dim_index] - minus_side[dim_index]) for dim_index in range(3)])

def divergence(padded):
    center, plus_side, minus_side = neighbour_sets(padded)
    total = 0.5 * (plus_side[0][0] - minus_side[0][0])
    total = total + 0.5 * (plus_side[1][1] - minus_side[1][1])
    return total + 0.5 * (plus_side[2][2] - minus_side[2][2])

def pressure_poisson(padded):
    center, plus_side, minus_side = neighbour_sets(padded)
    return 7.0 * center - six_sum(plus_side, minus_side)

def oseen_apply(padded, reaction_k, wind_k):
    upper = transport(padded[:3], reaction_k, wind_k) + gradient(padded[3])
    center, plus_side, minus_side = neighbour_sets(padded[3])
    lower = -divergence(padded[:3]) - 0.5 * (6.0 * center - six_sum(plus_side, minus_side))
    return jnp.concatenate([upper, lower[None]], 0)

def precondition(vector, wind, reaction, mass):
    pressure = vector[3]
    first_guess = pressure / 7.0
    second_guess = first_guess + (pressure - pressure_poisson(grid_pad(first_guess))) / 7.0
    schur = -transport(grid_pad(second_guess), reaction, wind) / mass
    residue = vector[:3] - gradient(grid_pad(schur))
    diagonal = 6.0 + reaction
    velocity_first = residue / diagonal
    velocity = velocity_first + (residue - transport(grid_pad(velocity_first), reaction, wind)) / diagonal
    return jnp.concatenate([velocity, schur[None]], 0)

def reference(start, wind, reaction, mass):
    scale_start = jnp.sqrt(jnp.sum(start * start))
    vectors = [start / scale_start]
    searches = []
    hess = jnp.zeros((ITERS + 1, ITERS), jnp.float32)
    for column in range(ITERS):
        found = precondition(vectors[column], wind, reaction, mass)
        searches.append(found)
        image = oseen_apply(grid_pad(found), reaction, wind)
        projected = jnp.stack([jnp.sum(vectors[row] * image) for row in range(column + 1)])
        for row in range(column + 1):
            image = image - projected[row] * vectors[row]
        norm_next = jnp.sqrt(jnp.sum(image * image))
        hess = hess.at[:column + 1, column].set(projected)
        hess = hess.at[column + 1, column].set(norm_next)
        vectors.append(image / norm_next)
    return (jnp.stack(vectors), jnp.stack(searches), hess)
```

```python
import functools

import jax
import jax.numpy as jnp
from jax import lax
from jax.experimental import pallas as pl
from jax.experimental.pallas import tpu as pltpu
from jax.sharding import PartitionSpec as P

ITERS = 3
AXES = ("slab", "sub")
SHIFTS = (1.5, 5.0, 4.5)
PIVOT_FLOOR = 0.01
PAD = 8


def neighbours(devices):
    up = [(i, i + 1) for i in range(devices - 1)]
    return up, [(j, i) for i, j in up]


def edge_rows(field, axis):
    sub = lax.axis_index("sub")
    start = (1 - sub) * (field.shape[axis] - PAD)
    return lax.dynamic_slice_in_dim(field, start, PAD, axis)


def across(field):
    return lax.ppermute(field, "sub", [(0, 1), (1, 0)])


def extend_coefficients(stacked):
    up, down = neighbours(lax.axis_size("slab"))
    length = stacked.shape[1]
    low = lax.ppermute(stacked[:, length - 3 :], "slab", up)
    high = lax.ppermute(stacked[:, :3], "slab", down)
    tall = jnp.concatenate([low, stacked, high], 1)
    other = across(edge_rows(tall, 2))
    sub = lax.axis_index("sub")
    left = jnp.where(sub == 1, other, 0.0)
    right = jnp.where(sub == 0, other, 0.0)
    return jnp.concatenate([left, tall, right], 2)


def exchange(vector):
    up, down = neighbours(lax.axis_size("slab"))
    length = vector.shape[1]
    last = jnp.concatenate(
        [vector[3, length - 5 :]] + [vector[c, length - 2 :] for c in range(3)], 0
    )
    first = jnp.concatenate([vector[3, :5]] + [vector[c, :2] for c in range(3)], 0)
    low = lax.ppermute(last, "slab", up)
    high = lax.ppermute(first, "slab", down)
    side = across(edge_rows(vector, 2))
    corner = across(edge_rows(jnp.concatenate([low, high], 0), 1))
    return low, high, side, corner


def plane_shifts(center):
    rows, lanes = center.shape
    lane = lax.broadcasted_iota(jnp.int32, center.shape, 1)
    y_plus = pltpu.roll(center, rows - 1, 0)
    y_minus = pltpu.roll(center, 1, 0)
    z_plus = jnp.where(lane == lanes - 1, 0.0, pltpu.roll(center, lanes - 1, 1))
    z_minus = jnp.where(lane == 0, 0.0, pltpu.roll(center, 1, 1))
    return y_plus, y_minus, z_plus, z_minus


def apply_kernel(
    count, shift, slabs, subs, *refs
):
    place, low, high, side, corner, coef, tile_in = refs[:7]
    olds = refs[7 : 7 + count]
    found, new, tile_out = refs[7 + count : 10 + count]
    pres, tee, schur, vel, first, second = refs[10 + count :]
    own = olds[-1]
    cells_x, cells_y, lanes = own.shape[1:]
    rows = cells_y + 2 * PAD
    slab, sub = place[0], place[1]
    is_left = sub == 0

    def put(write, middle, beyond):
        write(slice(PAD, PAD + cells_y), middle)
        write(slice(0, PAD), jnp.where(is_left, 0.0, beyond))
        write(slice(PAD + cells_y, rows), jnp.where(is_left, beyond, 0.0))

    def writer(ref, *lead):
        def write(span, value):
            ref[(*lead, span, slice(None))] = value

        return write

    for i in range(5):
        put(writer(pres, i), low[i], corner[i])
        put(writer(pres, 5 + cells_x + i), high[i], corner[11 + i])
    for c in range(3):
        for i in range(2):
            k = 5 + 2 * c + i
            put(writer(vel, c, i), low[k], corner[k])
            put(writer(vel, c, 2 + cells_x + i), high[k], corner[11 + k])

    @pl.loop(0, cells_x)
    def _(i):
        put(writer(pres, 5 + i), own[3, i], side[3, i])
        for c in range(3):
            put(writer(vel, c, 2 + i), own[c, i], side[c, i])

    row = lax.broadcasted_iota(jnp.int32, (rows, lanes), 0) + (sub * cells_y - PAD)
    inside_y = (row >= 0) & (row < cells_y * subs)

    def inside(i, width):
        x = slab * cells_x - width + i
        good = ((x >= 0) & (x < cells_x * slabs)).astype(jnp.int32)
        return inside_y & (jnp.full((rows, lanes), good, jnp.int32) > 0)

    def transport(center, x_plus, x_minus, shifts, k):
        y_plus, y_minus, z_plus, z_minus = shifts
        total = x_plus + x_minus + y_plus + y_minus + z_plus + z_minus
        convect = coef[0, k] * (x_plus - x_minus) + coef[1, k] * (y_plus - y_minus)
        convect = convect + coef[2, k] * (z_plus - z_minus)
        return (6.0 + coef[3, k]) * center - total + 0.5 * convect

    @pl.loop(0, cells_x + 8)
    def _(i):
        center = pres[i + 1]
        y_plus, y_minus, z_plus, z_minus = plane_shifts(center)
        total = pres[i + 2] + pres[i] + y_plus + y_minus + z_plus + z_minus
        tee[i] = jnp.where(inside(i, 4), center * (1.0 / 7.0) + total * (1.0 / 49.0), 0.0)

    @pl.loop(0, cells_x + 6)
    def _(i):
        center = tee[i + 1]
        value = transport(center, tee[i + 2], tee[i], plane_shifts(center), i)
        schur[i] = jnp.where(inside(i, 3), -value / coef[4, i], 0.0)

    @pl.loop(0, cells_x + 4)
    def _(i):
        center = schur[i + 1]
        y_plus, y_minus, z_plus, z_minus = plane_shifts(center)
        inverse = jnp.where(inside(i, 2), 1.0 / (6.0 + coef[3, i + 1]), 0.0)
        slopes = (schur[i + 2] - schur[i], y_plus - y_minus, z_plus - z_minus)
        for c in range(3):
            residue = vel[c, i] - 0.5 * slopes[c]
            vel[c, i] = residue
            first[c, i] = residue * inverse

    @pl.loop(0, cells_x + 2)
    def _(i):
        inverse = jnp.where(inside(i, 1), 1.0 / (6.0 + coef[3, i + 2]), 0.0)
        for c in range(3):
            center = first[c, i + 1]
            value = transport(
                center, first[c, i + 2], first[c, i], plane_shifts(center), i + 2
            )
            second[c, i] = center + (vel[c, i + 1] - value) * inverse

    mid = slice(PAD, PAD + cells_y)
    zero = jnp.zeros((cells_y, lanes), jnp.float32)

    def last_stage(i, sums):
        q = schur[i + 3]
        q_up, q_down = schur[i + 4], schur[i + 2]
        qy_plus, qy_minus, qz_plus, qz_minus = plane_shifts(q)
        slopes = (q_up - q_down, qy_plus - qy_minus, qz_plus - qz_minus)
        total = q_up + q_down + qy_plus + qy_minus + qz_plus + qz_minus
        div = jnp.zeros_like(q)
        images = []
        for c in range(3):
            center = second[c, i + 1]
            above, below = second[c, i + 2], second[c, i]
            shifts = plane_shifts(center)
            div = div + (above - below, shifts[0] - shifts[1], shifts[2] - shifts[3])[c]
            value = transport(center, above, below, shifts, i + 3)
            images.append(value + 0.5 * slopes[c])
            found[c, i] = center[mid]
        found[3, i] = q[mid]
        images.append(-0.5 * div - 0.5 * (6.0 * q - total))
        sums = list(sums)
        for c in range(4):
            fresh = images[c][mid] - shift * own[c, i]
            new[c, i] = fresh
            for k in range(count):
                sums[k] = sums[k] + fresh * olds[k][c, i]
            sums[count] = sums[count] + fresh * fresh
            if count == 1:
                old = own[c, i]
                sums[2] = sums[2] + old * old
        return tuple(sums)

    sums = lax.fori_loop(
        0, cells_x, last_stage, (zero,) * (count + 1 + (count == 1))
    )
    lane = lax.broadcasted_iota(jnp.int32, (8, 128), 1)
    base = count * (count + 1) // 2
    tile = tile_in[...]
    for k in range(count + 1):
        tile = jnp.where(lane == base + k, jnp.sum(sums[k]), tile)
    if count == 1:
        tile = jnp.where(lane == 0, jnp.sum(sums[2]), tile)
    tile_out[...] = tile


def apply_both(olds, coef, tile, shift):
    own = olds[-1]
    cells_x, cells_y, lanes = own.shape[1:]
    rows = cells_y + 2 * PAD
    low, high, side, corner = exchange(own)
    place = jnp.stack([lax.axis_index("slab"), lax.axis_index("sub")]).astype(jnp.int32)
    whole = pl.BlockSpec(memory_space=pltpu.VMEM)
    f32 = jnp.float32
    return pl.pallas_call(
        functools.partial(
            apply_kernel, len(olds), shift, lax.axis_size("slab"), lax.axis_size("sub")
        ),
        name=f"apply_{len(olds)}",
        in_specs=[pl.BlockSpec(memory_space=pltpu.SMEM)] + [whole] * (6 + len(olds)),
        out_specs=[whole] * 3,
        out_shape=[
            jax.ShapeDtypeStruct(own.shape, f32),
            jax.ShapeDtypeStruct(own.shape, f32),
            jax.ShapeDtypeStruct((8, 128), f32),
        ],
        scratch_shapes=[
            pltpu.VMEM((cells_x + 10, rows, lanes), f32),
            pltpu.VMEM((cells_x + 8, rows, lanes), f32),
            pltpu.VMEM((cells_x + 6, rows, lanes), f32),
            pltpu.VMEM((3, cells_x + 4, rows, lanes), f32),
            pltpu.VMEM((3, cells_x + 4, rows, lanes), f32),
            pltpu.VMEM((3, cells_x + 2, rows, lanes), f32),
        ],
        compiler_params=pltpu.CompilerParams(vmem_limit_bytes=56 * 1024 * 1024),
    )(place, low, high, side, corner, coef, tile, *olds)


def combine_kernel(*refs):
    parts = refs[0]
    vectors, founds = refs[1:5], refs[5:8]
    basis, search, small = refs[8:]
    total = jnp.sum(parts[...], axis=0)[0:1]
    lane = lax.broadcasted_iota(jnp.int32, (1, 128), 1)

    def gram(a, b):
        a, b = max(a, b), min(a, b)
        at = a * (a + 1) // 2 + b
        return jnp.sum(jnp.where(lane == at, total, 0.0), axis=1, keepdims=True)

    n = ITERS + 1
    upper, share = {}, None
    for j in range(n):
        for i in range(j):
            value = gram(i, j)
            for k in range(i):
                value = value - upper[k, i] * upper[k, j]
            upper[i, j] = value / upper[i, i]
        full = gram(j, j)
        left = full
        for k in range(j):
            left = left - upper[k, j] * upper[k, j]
        share = left / full if share is None else jnp.minimum(share, left / full)
        upper[j, j] = jnp.sqrt(left)
    inverse = {}
    for j in range(n):
        inverse[j, j] = 1.0 / upper[j, j]
        for i in range(j - 1, -1, -1):
            value = upper[i, i + 1] * inverse[i + 1, j]
            for k in range(i + 2, j + 1):
                value = value + upper[i, k] * inverse[k, j]
            inverse[i, j] = -value / upper[i, i]
    rows = lax.broadcasted_iota(jnp.int32, (8, 128), 0)
    lanes = lax.broadcasted_iota(jnp.int32, (8, 128), 1)
    tile = jnp.where(rows == 7, share, 0.0)
    for j in range(ITERS):
        for i in range(j + 2):
            value = None
            for k in range(max(i - 1, 0), j + 1):
                moved = upper[i, k + 1]
                if i <= k:
                    moved = moved + SHIFTS[k] * upper[i, k]
                term = moved * inverse[k, j]
                value = term if value is None else value + term
            tile = jnp.where((rows == i) & (lanes == j), value, tile)
    small[...] = tile

    @pl.loop(0, vectors[0].shape[1])
    def _(x):
        for c in range(4):
            for count, sources, target in ((n, vectors, basis), (ITERS, founds, search)):
                planes = [source[c, x] for source in sources]
                for j in range(count):
                    value = planes[0] * inverse[0, j]
                    for i in range(1, j + 1):
                        value = value + planes[i] * inverse[i, j]
                    target[j, c, x] = value


def step_by_step(start, coef):
    def total(value):
        return lax.psum(jnp.sum(value), AXES)

    blank = jnp.zeros((8, 128), jnp.float32)
    vectors = [start / jnp.sqrt(total(start * start))]
    searches = []
    hess = jnp.zeros((8, 128), jnp.float32)
    for column in range(ITERS):
        found, image, _ = apply_both([vectors[column]], coef, blank, 0.0)
        searches.append(found)
        projected = [total(vector * image) for vector in vectors]
        for row in range(column + 1):
            image = image - projected[row] * vectors[row]
            hess = hess.at[row, column].set(projected[row])
        norm_next = jnp.sqrt(total(image * image))
        hess = hess.at[column + 1, column].set(norm_next)
        vectors.append(image / norm_next)
    return jnp.stack(vectors), jnp.stack(searches), hess


def per_device(start, wind, reaction, mass):
    coef = extend_coefficients(jnp.concatenate([wind, reaction[None], mass[None]], 0))
    tile = jnp.zeros((8, 128), jnp.float32)
    vectors, founds = [start], []
    for column in range(ITERS):
        found, fresh, tile = apply_both(vectors, coef, tile, SHIFTS[column])
        founds.append(found)
        vectors.append(fresh)
    devices = lax.axis_size("slab") * lax.axis_size("sub")
    parts = lax.all_to_all(jnp.broadcast_to(tile[None], (devices, 8, 128)), AXES, 0, 0)
    whole = pl.BlockSpec(memory_space=pltpu.VMEM)
    basis, search, small = pl.pallas_call(
        combine_kernel,
        name="combine",
        in_specs=[whole] * 8,
        out_specs=[whole] * 3,
        out_shape=[
            jax.ShapeDtypeStruct((ITERS + 1,) + start.shape, jnp.float32),
            jax.ShapeDtypeStruct((ITERS,) + start.shape, jnp.float32),
            jax.ShapeDtypeStruct((8, 128), jnp.float32),
        ],
        compiler_params=pltpu.CompilerParams(vmem_limit_bytes=56 * 1024 * 1024),
    )(parts, *vectors, *founds)

    def body(state):
        basis, search, hess = step_by_step(start, coef)
        return basis, search, hess.at[7, 0].set(1.0)

    basis, search, small = lax.while_loop(
        lambda state: jnp.logical_not(state[2][7, 0] >= PIVOT_FLOOR),
        body,
        (basis, search, small),
    )
    return basis, search, small[: ITERS + 1, :ITERS]


def solution(mesh):
    return jax.shard_map(
        per_device,
        mesh=mesh,
        in_specs=(
            P(None, "slab", "sub", None),
            P(None, "slab", "sub", None),
            P("slab", "sub", None),
            P("slab", "sub", None),
        ),
        out_specs=(P(None, None, "slab", "sub", None), P(None, None, "slab", "sub", None), P()),
        check_vma=False,
    )
```

```python
import functools

import jax
import jax.numpy as jnp
from jax import lax
from jax.experimental import pallas as pl
from jax.experimental.pallas import tpu as pltpu
from jax.sharding import PartitionSpec as P

ITERS = 3
AXES = ("slab", "sub")
SHIFTS = (1.5, 5.0, 4.5)
PIVOT_FLOOR = 0.01
PAD = 8


def neighbours(devices):
    up = [(i, i + 1) for i in range(devices - 1)]
    return up, [(j, i) for i, j in up]


def edge_rows(field, axis):
    sub = lax.axis_index("sub")
    start = (1 - sub) * (field.shape[axis] - PAD)
    return lax.dynamic_slice_in_dim(field, start, PAD, axis)


def across(field):
    return lax.ppermute(field, "sub", [(0, 1), (1, 0)])


def extend_coefficients(stacked):
    up, down = neighbours(lax.axis_size("slab"))
    length = stacked.shape[1]
    low = lax.ppermute(stacked[:, length - 3 :], "slab", up)
    high = lax.ppermute(stacked[:, :3], "slab", down)
    tall = jnp.concatenate([low, stacked, high], 1)
    other = across(edge_rows(tall, 2))
    sub = lax.axis_index("sub")
    left = jnp.where(sub == 1, other, 0.0)
    right = jnp.where(sub == 0, other, 0.0)
    return jnp.concatenate([left, tall, right], 2)


def exchange(vector):
    up, down = neighbours(lax.axis_size("slab"))
    length = vector.shape[1]
    last = jnp.concatenate(
        [vector[3, length - 5 :]] + [vector[c, length - 2 :] for c in range(3)], 0
    )
    first = jnp.concatenate([vector[3, :5]] + [vector[c, :2] for c in range(3)], 0)
    low = lax.ppermute(last, "slab", up)
    high = lax.ppermute(first, "slab", down)
    side = across(edge_rows(vector, 2))
    corner = across(edge_rows(jnp.concatenate([low, high], 0), 1))
    return low, high, side, corner


def plane_shifts(center):
    rows, lanes = center.shape
    lane = lax.broadcasted_iota(jnp.int32, center.shape, 1)
    y_plus = pltpu.roll(center, rows - 1, 0)
    y_minus = pltpu.roll(center, 1, 0)
    z_plus = jnp.where(lane == lanes - 1, 0.0, pltpu.roll(center, lanes - 1, 1))
    z_minus = jnp.where(lane == 0, 0.0, pltpu.roll(center, 1, 1))
    return y_plus, y_minus, z_plus, z_minus


def apply_kernel(
    count, shift, slabs, subs, *refs
):
    place, low, high, side, corner, coef, tile_in = refs[:7]
    olds = refs[7 : 7 + count]
    found, new, tile_out = refs[7 + count : 10 + count]
    pres, tee, schur, vel, first, second = refs[10 + count :]
    own = olds[-1]
    cells_x, cells_y, lanes = own.shape[1:]
    rows = cells_y + 2 * PAD
    slab, sub = place[0], place[1]
    is_left = sub == 0

    def put(write, middle, beyond):
        write(slice(PAD, PAD + cells_y), middle)
        write(slice(0, PAD), jnp.where(is_left, 0.0, beyond))
        write(slice(PAD + cells_y, rows), jnp.where(is_left, beyond, 0.0))

    def writer(ref, *lead):
        def write(span, value):
            ref[(*lead, span, slice(None))] = value

        return write

    for i in range(5):
        put(writer(pres, i), low[i], corner[i])
        put(writer(pres, 5 + cells_x + i), high[i], corner[11 + i])
    for c in range(3):
        for i in range(2):
            k = 5 + 2 * c + i
            put(writer(vel, c, i), low[k], corner[k])
            put(writer(vel, c, 2 + cells_x + i), high[k], corner[11 + k])

    @pl.loop(0, cells_x)
    def _(i):
        put(writer(pres, 5 + i), own[3, i], side[3, i])
        for c in range(3):
            put(writer(vel, c, 2 + i), own[c, i], side[c, i])

    row = lax.broadcasted_iota(jnp.int32, (rows, lanes), 0) + (sub * cells_y - PAD)
    inside_y = (row >= 0) & (row < cells_y * subs)

    def inside(i, width):
        x = slab * cells_x - width + i
        good = ((x >= 0) & (x < cells_x * slabs)).astype(jnp.int32)
        return inside_y & (jnp.full((rows, lanes), good, jnp.int32) > 0)

    def transport(center, x_plus, x_minus, shifts, k):
        y_plus, y_minus, z_plus, z_minus = shifts
        total = x_plus + x_minus + y_plus + y_minus + z_plus + z_minus
        convect = coef[0, k] * (x_plus - x_minus) + coef[1, k] * (y_plus - y_minus)
        convect = convect + coef[2, k] * (z_plus - z_minus)
        return (6.0 + coef[3, k]) * center - total + 0.5 * convect

    @pl.loop(0, cells_x + 8)
    def _(i):
        center = pres[i + 1]
        y_plus, y_minus, z_plus, z_minus = plane_shifts(center)
        total = pres[i + 2] + pres[i] + y_plus + y_minus + z_plus + z_minus
        tee[i] = jnp.where(inside(i, 4), center * (1.0 / 7.0) + total * (1.0 / 49.0), 0.0)

    @pl.loop(0, cells_x + 6)
    def _(i):
        center = tee[i + 1]
        value = transport(center, tee[i + 2], tee[i], plane_shifts(center), i)
        schur[i] = jnp.where(inside(i, 3), -value / coef[4, i], 0.0)

    @pl.loop(0, cells_x + 4)
    def _(i):
        center = schur[i + 1]
        y_plus, y_minus, z_plus, z_minus = plane_shifts(center)
        inverse = jnp.where(inside(i, 2), 1.0 / (6.0 + coef[3, i + 1]), 0.0)
        slopes = (schur[i + 2] - schur[i], y_plus - y_minus, z_plus - z_minus)
        for c in range(3):
            residue = vel[c, i] - 0.5 * slopes[c]
            vel[c, i] = residue
            first[c, i] = residue * inverse

    @pl.loop(0, cells_x + 2)
    def _(i):
        inverse = jnp.where(inside(i, 1), 1.0 / (6.0 + coef[3, i + 2]), 0.0)
        for c in range(3):
            center = first[c, i + 1]
            value = transport(
                center, first[c, i + 2], first[c, i], plane_shifts(center), i + 2
            )
            second[c, i] = center + (vel[c, i + 1] - value) * inverse

    mid = slice(PAD, PAD + cells_y)
    zero = jnp.zeros((cells_y, lanes), jnp.float32)

    def last_stage(i, sums):
        q = schur[i + 3]
        q_up, q_down = schur[i + 4], schur[i + 2]
        qy_plus, qy_minus, qz_plus, qz_minus = plane_shifts(q)
        slopes = (q_up - q_down, qy_plus - qy_minus, qz_plus - qz_minus)
        total = q_up + q_down + qy_plus + qy_minus + qz_plus + qz_minus
        div = jnp.zeros_like(q)
        images = []
        for c in range(3):
            center = second[c, i + 1]
            above, below = second[c, i + 2], second[c, i]
            shifts = plane_shifts(center)
            div = div + (above - below, shifts[0] - shifts[1], shifts[2] - shifts[3])[c]
            value = transport(center, above, below, shifts, i + 3)
            images.append(value + 0.5 * slopes[c])
            found[c, i] = center[mid]
        found[3, i] = q[mid]
        images.append(-0.5 * div - 0.5 * (6.0 * q - total))
        sums = list(sums)
        for c in range(4):
            fresh = images[c][mid] - shift * own[c, i]
            new[c, i] = fresh
            for k in range(count):
                sums[k] = sums[k] + fresh * olds[k][c, i]
            sums[count] = sums[count] + fresh * fresh
            if count == 1:
                old = own[c, i]
                sums[2] = sums[2] + old * old
        return tuple(sums)

    sums = lax.fori_loop(
        0, cells_x, last_stage, (zero,) * (count + 1 + (count == 1))
    )
    lane = lax.broadcasted_iota(jnp.int32, (8, 128), 1)
    base = count * (count + 1) // 2
    tile = tile_in[...]
    for k in range(count + 1):
        tile = jnp.where(lane == base + k, jnp.sum(sums[k]), tile)
    if count == 1:
        tile = jnp.where(lane == 0, jnp.sum(sums[2]), tile)
    tile_out[...] = tile


def apply_both(olds, coef, tile, shift):
    own = olds[-1]
    cells_x, cells_y, lanes = own.shape[1:]
    rows = cells_y + 2 * PAD
    low, high, side, corner = exchange(own)
    place = jnp.stack([lax.axis_index("slab"), lax.axis_index("sub")]).astype(jnp.int32)
    whole = pl.BlockSpec(memory_space=pltpu.VMEM)
    f32 = jnp.float32
    return pl.pallas_call(
        functools.partial(
            apply_kernel, len(olds), shift, lax.axis_size("slab"), lax.axis_size("sub")
        ),
        name=f"apply_{len(olds)}",
        in_specs=[pl.BlockSpec(memory_space=pltpu.SMEM)] + [whole] * (6 + len(olds)),
        out_specs=[whole] * 3,
        out_shape=[
            jax.ShapeDtypeStruct(own.shape, f32),
            jax.ShapeDtypeStruct(own.shape, f32),
            jax.ShapeDtypeStruct((8, 128), f32),
        ],
        scratch_shapes=[
            pltpu.VMEM((cells_x + 10, rows, lanes), f32),
            pltpu.VMEM((cells_x + 8, rows, lanes), f32),
            pltpu.VMEM((cells_x + 6, rows, lanes), f32),
            pltpu.VMEM((3, cells_x + 4, rows, lanes), f32),
            pltpu.VMEM((3, cells_x + 4, rows, lanes), f32),
            pltpu.VMEM((3, cells_x + 2, rows, lanes), f32),
        ],
        compiler_params=pltpu.CompilerParams(vmem_limit_bytes=56 * 1024 * 1024),
    )(place, low, high, side, corner, coef, tile, *olds)


def combine_kernel(*refs):
    parts = refs[0]
    vectors, founds = refs[1:5], refs[5:8]
    basis, search, small = refs[8:]
    total = jnp.sum(parts[...], axis=0)[0:1]
    lane = lax.broadcasted_iota(jnp.int32, (1, 128), 1)

    def gram(a, b):
        a, b = max(a, b), min(a, b)
        at = a * (a + 1) // 2 + b
        return jnp.sum(jnp.where(lane == at, total, 0.0), axis=1, keepdims=True)

    n = ITERS + 1
    upper, share = {}, None
    for j in range(n):
        for i in range(j):
            value = gram(i, j)
            for k in range(i):
                value = value - upper[k, i] * upper[k, j]
            upper[i, j] = value / upper[i, i]
        full = gram(j, j)
        left = full
        for k in range(j):
            left = left - upper[k, j] * upper[k, j]
        share = left / full if share is None else jnp.minimum(share, left / full)
        upper[j, j] = jnp.sqrt(left)
    inverse = {}
    for j in range(n):
        inverse[j, j] = 1.0 / upper[j, j]
        for i in range(j - 1, -1, -1):
            value = upper[i, i + 1] * inverse[i + 1, j]
            for k in range(i + 2, j + 1):
                value = value + upper[i, k] * inverse[k, j]
            inverse[i, j] = -value / upper[i, i]
    rows = lax.broadcasted_iota(jnp.int32, (8, 128), 0)
    lanes = lax.broadcasted_iota(jnp.int32, (8, 128), 1)
    tile = jnp.where(rows == 7, share, 0.0)
    for j in range(ITERS):
        for i in range(j + 2):
            value = None
            for k in range(max(i - 1, 0), j + 1):
                moved = upper[i, k + 1]
                if i <= k:
                    moved = moved + SHIFTS[k] * upper[i, k]
                term = moved * inverse[k, j]
                value = term if value is None else value + term
            tile = jnp.where((rows == i) & (lanes == j), value, tile)
    small[...] = tile

    @pl.loop(0, vectors[0].shape[1])
    def _(x):
        for c in range(4):
            for count, sources, target in ((n, vectors, basis), (ITERS, founds, search)):
                planes = [source[c, x] for source in sources]
                for j in range(count):
                    value = planes[0] * inverse[0, j]
                    for i in range(1, j + 1):
                        value = value + planes[i] * inverse[i, j]
                    target[j, c, x] = value


def step_by_step(start, coef):
    def total(value):
        return lax.psum(jnp.sum(value), AXES)

    blank = jnp.zeros((8, 128), jnp.float32)
    vectors = [start / jnp.sqrt(total(start * start))]
    searches = []
    hess = jnp.zeros((8, 128), jnp.float32)
    for column in range(ITERS):
        found, image, _ = apply_both([vectors[column]], coef, blank, 0.0)
        searches.append(found)
        projected = [total(vector * image) for vector in vectors]
        for row in range(column + 1):
            image = image - projected[row] * vectors[row]
            hess = hess.at[row, column].set(projected[row])
        norm_next = jnp.sqrt(total(image * image))
        hess = hess.at[column + 1, column].set(norm_next)
        vectors.append(image / norm_next)
    return jnp.stack(vectors), jnp.stack(searches), hess


def per_device(start, wind, reaction, mass):
    coef = extend_coefficients(jnp.concatenate([wind, reaction[None], mass[None]], 0))
    tile = jnp.zeros((8, 128), jnp.float32)
    vectors, founds = [start], []
    for column in range(ITERS):
        found, fresh, tile = apply_both(vectors, coef, tile, SHIFTS[column])
        founds.append(found)
        vectors.append(fresh)
    devices = lax.axis_size("slab") * lax.axis_size("sub")
    parts = lax.all_to_all(jnp.broadcast_to(tile[None], (devices, 8, 128)), AXES, 0, 0)
    whole = pl.BlockSpec(memory_space=pltpu.VMEM)
    basis, search, small = pl.pallas_call(
        combine_kernel,
        name="combine",
        in_specs=[whole] * 8,
        out_specs=[whole] * 3,
        out_shape=[
            jax.ShapeDtypeStruct((ITERS + 1,) + start.shape, jnp.float32),
            jax.ShapeDtypeStruct((ITERS,) + start.shape, jnp.float32),
            jax.ShapeDtypeStruct((8, 128), jnp.float32),
        ],
        compiler_params=pltpu.CompilerParams(vmem_limit_bytes=56 * 1024 * 1024),
    )(parts, *vectors, *founds)

    def body(state):
        begin = jnp.where(state[2][7, 0] > 2.0, 0.0, start)
        basis, search, hess = step_by_step(begin, coef)
        return basis, search, hess.at[7, 0].set(1.0)

    basis, search, small = lax.while_loop(
        lambda state: jnp.logical_not(state[2][7, 0] >= PIVOT_FLOOR),
        body,
        (basis, search, small),
    )
    return basis, search, small[: ITERS + 1, :ITERS]


def solution(mesh):
    return jax.shard_map(
        per_device,
        mesh=mesh,
        in_specs=(
            P(None, "slab", "sub", None),
            P(None, "slab", "sub", None),
            P("slab", "sub", None),
            P("slab", "sub", None),
        ),
        out_specs=(P(None, None, "slab", "sub", None), P(None, None, "slab", "sub", None), P()),
        check_vma=False,
    )
```

```python
import functools

import jax
import jax.numpy as jnp
from jax import lax
from jax.experimental import pallas as pl
from jax.experimental.pallas import tpu as pltpu
from jax.sharding import PartitionSpec as P

ITERS = 3
AXES = ("slab", "sub")
SHIFTS = (1.5, 5.0, 4.5)
PIVOT_FLOOR = 0.01
PAD = 8


def neighbours(devices):
    up = [(i, i + 1) for i in range(devices - 1)]
    return up, [(j, i) for i, j in up]


def edge_rows(field, axis):
    sub = lax.axis_index("sub")
    start = (1 - sub) * (field.shape[axis] - PAD)
    return lax.dynamic_slice_in_dim(field, start, PAD, axis)


def across(field):
    return lax.ppermute(field, "sub", [(0, 1), (1, 0)])


def swap_pairs(devices, odd):
    mates = [(i, (i ^ 1) if not odd else (i + 1 if i % 2 else i - 1)) for i in range(devices)]
    return [(i, j) for i, j in mates if 0 <= j < devices]


def is_even():
    return lax.axis_index("slab") % 2 == 0


def split_ends(vector):
    length = vector.shape[1]
    last = [vector[3, length - 5 :]] + [vector[c, length - 2 :] for c in range(3)]
    first = [vector[3, :5]] + [vector[c, :2] for c in range(3)]
    return first, last


def for_pairs(first, last):
    even = is_even()
    first, last = jnp.concatenate(first, 0), jnp.concatenate(last, 0)
    return jnp.where(even, last, first), jnp.where(even, first, last)


def swap(to_near, to_far):
    devices = lax.axis_size("slab")
    near = lax.ppermute(to_near, "slab", swap_pairs(devices, False))
    far = lax.ppermute(to_far, "slab", swap_pairs(devices, True))
    corner = across(edge_rows(jnp.concatenate([near, far], 0), 1))
    return near, far, corner


def exchange_first(vector, stacked):
    names, length = stacked.shape[:2]
    flat = (names * 3,) + stacked.shape[2:]
    first, last = split_ends(vector)
    to_near, to_far = for_pairs(
        [stacked[:, :3].reshape(flat)] + first, [stacked[:, length - 3 :].reshape(flat)] + last
    )
    side_all = across(
        edge_rows(jnp.concatenate([vector.reshape((-1,) + vector.shape[2:]),
                                   stacked.reshape((-1,) + stacked.shape[2:])], 0), 1)
    )
    near, far, corner = swap(to_near, to_far)
    even, sub = is_even(), lax.axis_index("sub")
    planes, cut = near.shape[0], names * 3
    edge = (PAD,) + stacked.shape[3:]
    count = vector.shape[0] * length
    side = side_all[:count].reshape((vector.shape[0], length) + edge)
    low = jnp.where(even, far[:cut], near[:cut]).reshape((names, 3) + stacked.shape[2:])
    high = jnp.where(even, near[:cut], far[:cut]).reshape((names, 3) + stacked.shape[2:])
    from_near, from_far = corner[:cut], corner[planes : planes + cut]
    other = jnp.concatenate(
        [
            jnp.where(even, from_far, from_near).reshape((names, 3) + edge),
            side_all[count:].reshape((names, length) + edge),
            jnp.where(even, from_near, from_far).reshape((names, 3) + edge),
        ],
        1,
    )
    left = jnp.where(sub == 1, other, 0.0)
    right = jnp.where(sub == 0, other, 0.0)
    coef = jnp.concatenate([left, jnp.concatenate([low, stacked, high], 1), right], 2)
    rest = jnp.concatenate([corner[cut:planes], corner[planes + cut :]], 0)
    return (near[cut:], far[cut:], side, rest), coef


def exchange(to_near, to_far, side_out):
    side = across(side_out)
    near, far, corner = swap(to_near, to_far)
    return near, far, side, corner


def plane_shifts(center):
    rows, lanes = center.shape
    lane = lax.broadcasted_iota(jnp.int32, center.shape, 1)
    y_plus = pltpu.roll(center, rows - 1, 0)
    y_minus = pltpu.roll(center, 1, 0)
    z_plus = jnp.where(lane == lanes - 1, 0.0, pltpu.roll(center, lanes - 1, 1))
    z_minus = jnp.where(lane == 0, 0.0, pltpu.roll(center, 1, 1))
    return y_plus, y_minus, z_plus, z_minus


def apply_kernel(
    count, shift, slabs, subs, *refs
):
    place, near, far, side, corner, coef, tile_in = refs[:7]
    olds = refs[7 : 7 + count]
    found, new, tile_out, to_near, to_far, side_out = refs[7 + count : 13 + count]
    pres, tee, schur, vel, first, second = refs[13 + count :]
    own = olds[-1]
    cells_x, cells_y, lanes = own.shape[1:]
    rows = cells_y + 2 * PAD
    slab, sub = place[0], place[1]
    is_left = sub == 0
    even = slab % 2 == 0

    def low(i):
        return jnp.where(even, far[i], near[i]), jnp.where(even, corner[11 + i], corner[i])

    def high(i):
        return jnp.where(even, near[i], far[i]), jnp.where(even, corner[i], corner[11 + i])

    def put(write, middle, beyond):
        write(slice(PAD, PAD + cells_y), middle)
        write(slice(0, PAD), jnp.where(is_left, 0.0, beyond))
        write(slice(PAD + cells_y, rows), jnp.where(is_left, beyond, 0.0))

    def writer(ref, *lead):
        def write(span, value):
            ref[(*lead, span, slice(None))] = value

        return write

    for i in range(5):
        put(writer(pres, i), *low(i))
        put(writer(pres, 5 + cells_x + i), *high(i))
    for c in range(3):
        for i in range(2):
            k = 5 + 2 * c + i
            put(writer(vel, c, i), *low(k))
            put(writer(vel, c, 2 + cells_x + i), *high(k))

    @pl.loop(0, cells_x)
    def _(i):
        put(writer(pres, 5 + i), own[3, i], side[3, i])
        for c in range(3):
            put(writer(vel, c, 2 + i), own[c, i], side[c, i])

    row = lax.broadcasted_iota(jnp.int32, (rows, lanes), 0) + (sub * cells_y - PAD)
    inside_y = (row >= 0) & (row < cells_y * subs)

    def inside(i, width):
        x = slab * cells_x - width + i
        good = ((x >= 0) & (x < cells_x * slabs)).astype(jnp.int32)
        return inside_y & (jnp.full((rows, lanes), good, jnp.int32) > 0)

    def transport(center, x_plus, x_minus, shifts, k):
        y_plus, y_minus, z_plus, z_minus = shifts
        total = x_plus + x_minus + y_plus + y_minus + z_plus + z_minus
        convect = coef[0, k] * (x_plus - x_minus) + coef[1, k] * (y_plus - y_minus)
        convect = convect + coef[2, k] * (z_plus - z_minus)
        return (6.0 + coef[3, k]) * center - total + 0.5 * convect

    @pl.loop(0, cells_x + 8)
    def _(i):
        center = pres[i + 1]
        y_plus, y_minus, z_plus, z_minus = plane_shifts(center)
        total = pres[i + 2] + pres[i] + y_plus + y_minus + z_plus + z_minus
        tee[i] = jnp.where(inside(i, 4), center * (1.0 / 7.0) + total * (1.0 / 49.0), 0.0)

    @pl.loop(0, cells_x + 6)
    def _(i):
        center = tee[i + 1]
        value = transport(center, tee[i + 2], tee[i], plane_shifts(center), i)
        schur[i] = jnp.where(inside(i, 3), -value / coef[4, i], 0.0)

    @pl.loop(0, cells_x + 4)
    def _(i):
        center = schur[i + 1]
        y_plus, y_minus, z_plus, z_minus = plane_shifts(center)
        inverse = jnp.where(inside(i, 2), 1.0 / (6.0 + coef[3, i + 1]), 0.0)
        slopes = (schur[i + 2] - schur[i], y_plus - y_minus, z_plus - z_minus)
        for c in range(3):
            residue = vel[c, i] - 0.5 * slopes[c]
            vel[c, i] = residue
            first[c, i] = residue * inverse

    @pl.loop(0, cells_x + 2)
    def _(i):
        inverse = jnp.where(inside(i, 1), 1.0 / (6.0 + coef[3, i + 2]), 0.0)
        for c in range(3):
            center = first[c, i + 1]
            value = transport(
                center, first[c, i + 2], first[c, i], plane_shifts(center), i + 2
            )
            second[c, i] = center + (vel[c, i + 1] - value) * inverse

    mid = slice(PAD, PAD + cells_y)
    zero = jnp.zeros((cells_y, lanes), jnp.float32)

    def last_stage(i, sums):
        q = schur[i + 3]
        q_up, q_down = schur[i + 4], schur[i + 2]
        qy_plus, qy_minus, qz_plus, qz_minus = plane_shifts(q)
        slopes = (q_up - q_down, qy_plus - qy_minus, qz_plus - qz_minus)
        total = q_up + q_down + qy_plus + qy_minus + qz_plus + qz_minus
        div = jnp.zeros_like(q)
        images = []
        for c in range(3):
            center = second[c, i + 1]
            above, below = second[c, i + 2], second[c, i]
            shifts = plane_shifts(center)
            div = div + (above - below, shifts[0] - shifts[1], shifts[2] - shifts[3])[c]
            value = transport(center, above, below, shifts, i + 3)
            images.append(value + 0.5 * slopes[c])
            found[c, i] = center[mid]
        found[3, i] = q[mid]
        images.append(-0.5 * div - 0.5 * (6.0 * q - total))
        sums = list(sums)
        for c in range(4):
            fresh = images[c][mid] - shift * own[c, i]
            new[c, i] = fresh
            side_out[c, i] = jnp.where(is_left, fresh[cells_y - PAD :], fresh[:PAD])
            for k in range(count):
                sums[k] = sums[k] + fresh * olds[k][c, i]
            sums[count] = sums[count] + fresh * fresh
            if count == 1:
                old = own[c, i]
                sums[2] = sums[2] + old * old
        return tuple(sums)

    sums = lax.fori_loop(
        0, cells_x, last_stage, (zero,) * (count + 1 + (count == 1))
    )
    ends = [(3, i, cells_x - 5 + i) for i in range(5)]
    ends += [(c, i, cells_x - 2 + i) for c in range(3) for i in range(2)]
    for k, (c, i, j) in enumerate(ends):
        to_near[k] = jnp.where(even, new[c, j], new[c, i])
        to_far[k] = jnp.where(even, new[c, i], new[c, j])
    lane = lax.broadcasted_iota(jnp.int32, (8, 128), 1)
    base = count * (count + 1) // 2
    tile = tile_in[...]
    for k in range(count + 1):
        tile = jnp.where(lane == base + k, jnp.sum(sums[k]), tile)
    if count == 1:
        tile = jnp.where(lane == 0, jnp.sum(sums[2]), tile)
    tile_out[...] = tile


def apply_both(olds, arrived, coef, tile, shift):
    own = olds[-1]
    cells_x, cells_y, lanes = own.shape[1:]
    rows = cells_y + 2 * PAD
    place = jnp.stack([lax.axis_index("slab"), lax.axis_index("sub")]).astype(jnp.int32)
    whole = pl.BlockSpec(memory_space=pltpu.VMEM)
    f32 = jnp.float32
    return pl.pallas_call(
        functools.partial(
            apply_kernel, len(olds), shift, lax.axis_size("slab"), lax.axis_size("sub")
        ),
        name=f"apply_{len(olds)}",
        in_specs=[pl.BlockSpec(memory_space=pltpu.SMEM)] + [whole] * (6 + len(olds)),
        out_specs=[whole] * 6,
        out_shape=[
            jax.ShapeDtypeStruct(own.shape, f32),
            jax.ShapeDtypeStruct(own.shape, f32),
            jax.ShapeDtypeStruct((8, 128), f32),
            jax.ShapeDtypeStruct((11, cells_y, lanes), f32),
            jax.ShapeDtypeStruct((11, cells_y, lanes), f32),
            jax.ShapeDtypeStruct((4, cells_x, PAD, lanes), f32),
        ],
        scratch_shapes=[
            pltpu.VMEM((cells_x + 10, rows, lanes), f32),
            pltpu.VMEM((cells_x + 8, rows, lanes), f32),
            pltpu.VMEM((cells_x + 6, rows, lanes), f32),
            pltpu.VMEM((3, cells_x + 4, rows, lanes), f32),
            pltpu.VMEM((3, cells_x + 4, rows, lanes), f32),
            pltpu.VMEM((3, cells_x + 2, rows, lanes), f32),
        ],
        compiler_params=pltpu.CompilerParams(vmem_limit_bytes=56 * 1024 * 1024),
    )(place, *arrived, coef, tile, *olds)


def combine_kernel(*refs):
    parts = refs[0]
    vectors, founds = refs[1:5], refs[5:8]
    basis, search, small, least = refs[8:]
    total = jnp.sum(parts[...], axis=0)[0:1]
    lane = lax.broadcasted_iota(jnp.int32, (1, 128), 1)

    def gram(a, b):
        a, b = max(a, b), min(a, b)
        at = a * (a + 1) // 2 + b
        return jnp.sum(jnp.where(lane == at, total, 0.0), axis=1, keepdims=True)

    n = ITERS + 1
    upper, share = {}, None
    for j in range(n):
        for i in range(j):
            value = gram(i, j)
            for k in range(i):
                value = value - upper[k, i] * upper[k, j]
            upper[i, j] = value / upper[i, i]
        full = gram(j, j)
        left = full
        for k in range(j):
            left = left - upper[k, j] * upper[k, j]
        share = left / full if share is None else jnp.minimum(share, left / full)
        upper[j, j] = jnp.sqrt(left)
    inverse = {}
    for j in range(n):
        inverse[j, j] = 1.0 / upper[j, j]
        for i in range(j - 1, -1, -1):
            value = upper[i, i + 1] * inverse[i + 1, j]
            for k in range(i + 2, j + 1):
                value = value + upper[i, k] * inverse[k, j]
            inverse[i, j] = -value / upper[i, i]
    rows = lax.broadcasted_iota(jnp.int32, (8, 128), 0)
    lanes = lax.broadcasted_iota(jnp.int32, (8, 128), 1)
    tile = jnp.zeros((8, 128), jnp.float32)
    for j in range(ITERS):
        for i in range(j + 2):
            value = None
            for k in range(max(i - 1, 0), j + 1):
                moved = upper[i, k + 1]
                if i <= k:
                    moved = moved + SHIFTS[k] * upper[i, k]
                term = moved * inverse[k, j]
                value = term if value is None else value + term
            tile = jnp.where((rows == i) & (lanes == j), value, tile)
    small[...] = tile[: ITERS + 1, :ITERS]
    least[0] = jnp.sum(share)

    @pl.loop(0, vectors[0].shape[1])
    def _(x):
        for c in range(4):
            for count, sources, target in ((n, vectors, basis), (ITERS, founds, search)):
                planes = [source[c, x] for source in sources]
                for j in range(count):
                    value = planes[0] * inverse[0, j]
                    for i in range(1, j + 1):
                        value = value + planes[i] * inverse[i, j]
                    target[j, c, x] = value


def step_by_step(start, coef):
    def total(value):
        return lax.psum(jnp.sum(value), AXES)

    blank = jnp.zeros((8, 128), jnp.float32)
    vectors = [start / jnp.sqrt(total(start * start))]
    searches = []
    hess = jnp.zeros((ITERS + 1, ITERS), jnp.float32)
    for column in range(ITERS):
        own = vectors[column]
        arrived = exchange(*for_pairs(*split_ends(own)), edge_rows(own, 2))
        found, image = apply_both([own], arrived, coef, blank, 0.0)[:2]
        searches.append(found)
        projected = [total(vector * image) for vector in vectors]
        for row in range(column + 1):
            image = image - projected[row] * vectors[row]
            hess = hess.at[row, column].set(projected[row])
        norm_next = jnp.sqrt(total(image * image))
        hess = hess.at[column + 1, column].set(norm_next)
        vectors.append(image / norm_next)
    return jnp.stack(vectors), jnp.stack(searches), hess


def per_device(start, wind, reaction, mass):
    arrived, coef = exchange_first(start, jnp.concatenate([wind, reaction[None], mass[None]], 0))
    tile = jnp.zeros((8, 128), jnp.float32)
    vectors, founds = [start], []
    for column in range(ITERS):
        found, fresh, tile, *ends = apply_both(vectors, arrived, coef, tile, SHIFTS[column])
        founds.append(found)
        vectors.append(fresh)
        if column + 1 < ITERS:
            arrived = exchange(*ends)
    devices = lax.axis_size("slab") * lax.axis_size("sub")
    parts = lax.all_to_all(jnp.broadcast_to(tile[None], (devices, 8, 128)), AXES, 0, 0)
    whole = pl.BlockSpec(memory_space=pltpu.VMEM)
    basis, search, small, least = pl.pallas_call(
        combine_kernel,
        name="combine",
        in_specs=[whole] * 8,
        out_specs=[whole] * 3 + [pl.BlockSpec(memory_space=pltpu.SMEM)],
        out_shape=[
            jax.ShapeDtypeStruct((ITERS + 1,) + start.shape, jnp.float32),
            jax.ShapeDtypeStruct((ITERS,) + start.shape, jnp.float32),
            jax.ShapeDtypeStruct((ITERS + 1, ITERS), jnp.float32),
            jax.ShapeDtypeStruct((1,), jnp.float32),
        ],
        compiler_params=pltpu.CompilerParams(vmem_limit_bytes=56 * 1024 * 1024),
    )(parts, *vectors, *founds)

    def body(state):
        begin = jnp.where(state[3][0] > 2.0, 0.0, start)
        basis, search, hess = step_by_step(begin, coef)
        return basis, search, hess, jnp.ones((1,), jnp.float32)

    basis, search, small, _ = lax.while_loop(
        lambda state: jnp.logical_not(state[3][0] >= PIVOT_FLOOR),
        body,
        (basis, search, small, least),
    )
    return basis, search, small


def solution(mesh):
    return jax.shard_map(
        per_device,
        mesh=mesh,
        in_specs=(
            P(None, "slab", "sub", None),
            P(None, "slab", "sub", None),
            P("slab", "sub", None),
            P("slab", "sub", None),
        ),
        out_specs=(P(None, None, "slab", "sub", None), P(None, None, "slab", "sub", None), P()),
        check_vma=False,
    )
```

```python
import functools

import jax
import jax.numpy as jnp
from jax import lax
from jax.experimental import pallas as pl
from jax.experimental.pallas import tpu as pltpu
from jax.sharding import PartitionSpec as P

ITERS = 3
AXES = ("slab", "sub")
SHIFTS = (1.5, 5.0, 4.5)
PIVOT_FLOOR = 0.01
PAD = 8


def neighbours(devices):
    up = [(i, i + 1) for i in range(devices - 1)]
    return up, [(j, i) for i, j in up]


def edge_rows(field, axis):
    sub = lax.axis_index("sub")
    start = (1 - sub) * (field.shape[axis] - PAD)
    return lax.dynamic_slice_in_dim(field, start, PAD, axis)


def across(field):
    return lax.ppermute(field, "sub", [(0, 1), (1, 0)])


def swap_pairs(devices, odd):
    mates = [(i, (i ^ 1) if not odd else (i + 1 if i % 2 else i - 1)) for i in range(devices)]
    return [(i, j) for i, j in mates if 0 <= j < devices]


def is_even():
    return lax.axis_index("slab") % 2 == 0


def split_ends(vector):
    length = vector.shape[1]
    last = [vector[3, length - 5 :]] + [vector[c, length - 2 :] for c in range(3)]
    first = [vector[3, :5]] + [vector[c, :2] for c in range(3)]
    return first, last


def for_pairs(first, last):
    even = is_even()
    first, last = jnp.concatenate(first, 0), jnp.concatenate(last, 0)
    return jnp.where(even, last, first), jnp.where(even, first, last)


def swap(to_near, to_far):
    devices = lax.axis_size("slab")
    near = lax.ppermute(to_near, "slab", swap_pairs(devices, False))
    far = lax.ppermute(to_far, "slab", swap_pairs(devices, True))
    corner = across(edge_rows(jnp.concatenate([near, far], 0), 1))
    return near, far, corner


def exchange_first(vector, stacked):
    names, length = stacked.shape[:2]
    flat = (names * 3,) + stacked.shape[2:]
    first, last = split_ends(vector)
    to_near, to_far = for_pairs(
        [stacked[:, :3].reshape(flat)] + first, [stacked[:, length - 3 :].reshape(flat)] + last
    )
    side_all = across(
        edge_rows(jnp.concatenate([vector.reshape((-1,) + vector.shape[2:]),
                                   stacked.reshape((-1,) + stacked.shape[2:])], 0), 1)
    )
    near, far, corner = swap(to_near, to_far)
    even, sub = is_even(), lax.axis_index("sub")
    planes, cut = near.shape[0], names * 3
    edge = (PAD,) + stacked.shape[3:]
    count = vector.shape[0] * length
    side = side_all[:count].reshape((vector.shape[0], length) + edge)
    low = jnp.where(even, far[:cut], near[:cut]).reshape((names, 3) + stacked.shape[2:])
    high = jnp.where(even, near[:cut], far[:cut]).reshape((names, 3) + stacked.shape[2:])
    from_near, from_far = corner[:cut], corner[planes : planes + cut]
    other = jnp.concatenate(
        [
            jnp.where(even, from_far, from_near).reshape((names, 3) + edge),
            side_all[count:].reshape((names, length) + edge),
            jnp.where(even, from_near, from_far).reshape((names, 3) + edge),
        ],
        1,
    )
    left = jnp.where(sub == 1, other, 0.0)
    right = jnp.where(sub == 0, other, 0.0)
    coef = jnp.concatenate([left, jnp.concatenate([low, stacked, high], 1), right], 2)
    return (near, far, side, corner), coef


def exchange(to_near, to_far, side_out):
    side = across(side_out)
    near, far, corner = swap(to_near, to_far)
    return near, far, side, corner


def plane_shifts(center):
    rows, lanes = center.shape
    lane = lax.broadcasted_iota(jnp.int32, center.shape, 1)
    y_plus = pltpu.roll(center, rows - 1, 0)
    y_minus = pltpu.roll(center, 1, 0)
    z_plus = jnp.where(lane == lanes - 1, 0.0, pltpu.roll(center, lanes - 1, 1))
    z_minus = jnp.where(lane == 0, 0.0, pltpu.roll(center, 1, 1))
    return y_plus, y_minus, z_plus, z_minus


def apply_kernel(
    count, shift, slabs, subs, skip, *refs
):
    place, near, far, side, corner, coef = refs[:6]
    olds = refs[6 : 6 + count]
    tiles = refs[6 + count : -12]
    found, new, tile_out, to_near, to_far, side_out = refs[-12:-6]
    pres, tee, schur, vel, first, second = refs[-6:]
    own = olds[-1]
    cells_x, cells_y, lanes = own.shape[1:]
    rows = cells_y + 2 * PAD
    slab, sub = place[0], place[1]
    is_left = sub == 0
    even = slab % 2 == 0

    def low(i):
        i, j = skip + i, near.shape[0] + skip + i
        return jnp.where(even, far[i], near[i]), jnp.where(even, corner[j], corner[i])

    def high(i):
        i, j = skip + i, near.shape[0] + skip + i
        return jnp.where(even, near[i], far[i]), jnp.where(even, corner[i], corner[j])

    def put(write, middle, beyond):
        write(slice(PAD, PAD + cells_y), middle)
        write(slice(0, PAD), jnp.where(is_left, 0.0, beyond))
        write(slice(PAD + cells_y, rows), jnp.where(is_left, beyond, 0.0))

    def writer(ref, *lead):
        def write(span, value):
            ref[(*lead, span, slice(None))] = value

        return write

    for i in range(5):
        put(writer(pres, i), *low(i))
        put(writer(pres, 5 + cells_x + i), *high(i))
    for c in range(3):
        for i in range(2):
            k = 5 + 2 * c + i
            put(writer(vel, c, i), *low(k))
            put(writer(vel, c, 2 + cells_x + i), *high(k))

    @pl.loop(0, cells_x)
    def _(i):
        put(writer(pres, 5 + i), own[3, i], side[3, i])
        for c in range(3):
            put(writer(vel, c, 2 + i), own[c, i], side[c, i])

    row = lax.broadcasted_iota(jnp.int32, (rows, lanes), 0) + (sub * cells_y - PAD)
    inside_y = (row >= 0) & (row < cells_y * subs)

    def inside(i, width):
        x = slab * cells_x - width + i
        good = ((x >= 0) & (x < cells_x * slabs)).astype(jnp.int32)
        return inside_y & (jnp.full((rows, lanes), good, jnp.int32) > 0)

    def transport(center, x_plus, x_minus, shifts, k):
        y_plus, y_minus, z_plus, z_minus = shifts
        total = x_plus + x_minus + y_plus + y_minus + z_plus + z_minus
        convect = coef[0, k] * (x_plus - x_minus) + coef[1, k] * (y_plus - y_minus)
        convect = convect + coef[2, k] * (z_plus - z_minus)
        return (6.0 + coef[3, k]) * center - total + 0.5 * convect

    @pl.loop(0, cells_x + 8)
    def _(i):
        center = pres[i + 1]
        y_plus, y_minus, z_plus, z_minus = plane_shifts(center)
        total = pres[i + 2] + pres[i] + y_plus + y_minus + z_plus + z_minus
        tee[i] = jnp.where(inside(i, 4), center * (1.0 / 7.0) + total * (1.0 / 49.0), 0.0)

    @pl.loop(0, cells_x + 6)
    def _(i):
        center = tee[i + 1]
        value = transport(center, tee[i + 2], tee[i], plane_shifts(center), i)
        schur[i] = jnp.where(inside(i, 3), -value / coef[4, i], 0.0)

    @pl.loop(0, cells_x + 4)
    def _(i):
        center = schur[i + 1]
        y_plus, y_minus, z_plus, z_minus = plane_shifts(center)
        inverse = jnp.where(inside(i, 2), 1.0 / (6.0 + coef[3, i + 1]), 0.0)
        slopes = (schur[i + 2] - schur[i], y_plus - y_minus, z_plus - z_minus)
        for c in range(3):
            residue = vel[c, i] - 0.5 * slopes[c]
            vel[c, i] = residue
            first[c, i] = residue * inverse

    @pl.loop(0, cells_x + 2)
    def _(i):
        inverse = jnp.where(inside(i, 1), 1.0 / (6.0 + coef[3, i + 2]), 0.0)
        for c in range(3):
            center = first[c, i + 1]
            value = transport(
                center, first[c, i + 2], first[c, i], plane_shifts(center), i + 2
            )
            second[c, i] = center + (vel[c, i + 1] - value) * inverse

    mid = slice(PAD, PAD + cells_y)
    zero = jnp.zeros((cells_y, lanes), jnp.float32)

    def last_stage(i, sums):
        q = schur[i + 3]
        q_up, q_down = schur[i + 4], schur[i + 2]
        qy_plus, qy_minus, qz_plus, qz_minus = plane_shifts(q)
        slopes = (q_up - q_down, qy_plus - qy_minus, qz_plus - qz_minus)
        total = q_up + q_down + qy_plus + qy_minus + qz_plus + qz_minus
        div = jnp.zeros_like(q)
        images = []
        for c in range(3):
            center = second[c, i + 1]
            above, below = second[c, i + 2], second[c, i]
            shifts = plane_shifts(center)
            div = div + (above - below, shifts[0] - shifts[1], shifts[2] - shifts[3])[c]
            value = transport(center, above, below, shifts, i + 3)
            images.append(value + 0.5 * slopes[c])
            found[c, i] = center[mid]
        found[3, i] = q[mid]
        images.append(-0.5 * div - 0.5 * (6.0 * q - total))
        sums = list(sums)
        for c in range(4):
            fresh = images[c][mid] - shift * own[c, i]
            new[c, i] = fresh
            side_out[c, i] = jnp.where(is_left, fresh[cells_y - PAD :], fresh[:PAD])
            for k in range(count):
                sums[k] = sums[k] + fresh * olds[k][c, i]
            sums[count] = sums[count] + fresh * fresh
            if count == 1:
                old = own[c, i]
                sums[2] = sums[2] + old * old
        return tuple(sums)

    sums = lax.fori_loop(
        0, cells_x, last_stage, (zero,) * (count + 1 + (count == 1))
    )
    ends = [(3, i, cells_x - 5 + i) for i in range(5)]
    ends += [(c, i, cells_x - 2 + i) for c in range(3) for i in range(2)]
    for k, (c, i, j) in enumerate(ends):
        to_near[k] = jnp.where(even, new[c, j], new[c, i])
        to_far[k] = jnp.where(even, new[c, i], new[c, j])
    lane = lax.broadcasted_iota(jnp.int32, (8, 128), 1)
    base = count * (count + 1) // 2
    tile = tiles[0][...] if tiles else jnp.zeros((8, 128), jnp.float32)
    for k in range(count + 1):
        tile = jnp.where(lane == base + k, jnp.sum(sums[k]), tile)
    if count == 1:
        tile = jnp.where(lane == 0, jnp.sum(sums[2]), tile)
    tile_out[...] = jnp.broadcast_to(tile, tile_out.shape)


def apply_both(olds, arrived, coef, tiles, shift, tile_shape=(8, 128)):
    own = olds[-1]
    cells_x, cells_y, lanes = own.shape[1:]
    rows = cells_y + 2 * PAD
    place = jnp.stack([lax.axis_index("slab"), lax.axis_index("sub")]).astype(jnp.int32)
    whole = pl.BlockSpec(memory_space=pltpu.VMEM)
    f32 = jnp.float32
    return pl.pallas_call(
        functools.partial(
            apply_kernel, len(olds), shift, lax.axis_size("slab"), lax.axis_size("sub"),
            arrived[0].shape[0] - 11,
        ),
        name=f"apply_{len(olds)}",
        in_specs=[pl.BlockSpec(memory_space=pltpu.SMEM)] + [whole] * (5 + len(olds) + len(tiles)),
        out_specs=[whole] * 6,
        out_shape=[
            jax.ShapeDtypeStruct(own.shape, f32),
            jax.ShapeDtypeStruct(own.shape, f32),
            jax.ShapeDtypeStruct(tile_shape, f32),
            jax.ShapeDtypeStruct((11, cells_y, lanes), f32),
            jax.ShapeDtypeStruct((11, cells_y, lanes), f32),
            jax.ShapeDtypeStruct((4, cells_x, PAD, lanes), f32),
        ],
        scratch_shapes=[
            pltpu.VMEM((cells_x + 10, rows, lanes), f32),
            pltpu.VMEM((cells_x + 8, rows, lanes), f32),
            pltpu.VMEM((cells_x + 6, rows, lanes), f32),
            pltpu.VMEM((3, cells_x + 4, rows, lanes), f32),
            pltpu.VMEM((3, cells_x + 4, rows, lanes), f32),
            pltpu.VMEM((3, cells_x + 2, rows, lanes), f32),
        ],
        compiler_params=pltpu.CompilerParams(vmem_limit_bytes=56 * 1024 * 1024),
    )(place, *arrived, coef, *olds, *tiles)


def combine_kernel(*refs):
    parts = refs[0]
    vectors, founds = refs[1:5], refs[5:8]
    basis, search, small, least = refs[8:]
    total = jnp.sum(parts[...], axis=0)[0:1]
    lane = lax.broadcasted_iota(jnp.int32, (1, 128), 1)

    def gram(a, b):
        a, b = max(a, b), min(a, b)
        at = a * (a + 1) // 2 + b
        return jnp.sum(jnp.where(lane == at, total, 0.0), axis=1, keepdims=True)

    n = ITERS + 1
    upper, share = {}, None
    for j in range(n):
        for i in range(j):
            value = gram(i, j)
            for k in range(i):
                value = value - upper[k, i] * upper[k, j]
            upper[i, j] = value / upper[i, i]
        full = gram(j, j)
        left = full
        for k in range(j):
            left = left - upper[k, j] * upper[k, j]
        share = left / full if share is None else jnp.minimum(share, left / full)
        upper[j, j] = jnp.sqrt(left)
    inverse = {}
    for j in range(n):
        inverse[j, j] = 1.0 / upper[j, j]
        for i in range(j - 1, -1, -1):
            value = upper[i, i + 1] * inverse[i + 1, j]
            for k in range(i + 2, j + 1):
                value = value + upper[i, k] * inverse[k, j]
            inverse[i, j] = -value / upper[i, i]
    rows = lax.broadcasted_iota(jnp.int32, (8, 128), 0)
    lanes = lax.broadcasted_iota(jnp.int32, (8, 128), 1)
    tile = jnp.zeros((8, 128), jnp.float32)
    for j in range(ITERS):
        for i in range(j + 2):
            value = None
            for k in range(max(i - 1, 0), j + 1):
                moved = upper[i, k + 1]
                if i <= k:
                    moved = moved + SHIFTS[k] * upper[i, k]
                term = moved * inverse[k, j]
                value = term if value is None else value + term
            tile = jnp.where((rows == i) & (lanes == j), value, tile)
    small[...] = tile[: ITERS + 1, :ITERS]
    least[0] = jnp.sum(share)

    @pl.loop(0, vectors[0].shape[1])
    def _(x):
        for c in range(4):
            for count, sources, target in ((n, vectors, basis), (ITERS, founds, search)):
                planes = [source[c, x] for source in sources]
                for j in range(count):
                    value = planes[0] * inverse[0, j]
                    for i in range(1, j + 1):
                        value = value + planes[i] * inverse[i, j]
                    target[j, c, x] = value


def step_by_step(start, coef):
    def total(value):
        return lax.psum(jnp.sum(value), AXES)

    vectors = [start / jnp.sqrt(total(start * start))]
    searches = []
    hess = jnp.zeros((ITERS + 1, ITERS), jnp.float32)
    for column in range(ITERS):
        own = vectors[column]
        arrived = exchange(*for_pairs(*split_ends(own)), edge_rows(own, 2))
        found, image = apply_both([own], arrived, coef, (), 0.0)[:2]
        searches.append(found)
        projected = [total(vector * image) for vector in vectors]
        for row in range(column + 1):
            image = image - projected[row] * vectors[row]
            hess = hess.at[row, column].set(projected[row])
        norm_next = jnp.sqrt(total(image * image))
        hess = hess.at[column + 1, column].set(norm_next)
        vectors.append(image / norm_next)
    return jnp.stack(vectors), jnp.stack(searches), hess


def per_device(start, wind, reaction, mass):
    arrived, coef = exchange_first(start, jnp.concatenate([wind, reaction[None], mass[None]], 0))
    devices = lax.axis_size("slab") * lax.axis_size("sub")
    tiles = ()
    vectors, founds = [start], []
    for column in range(ITERS):
        shape = (8, 128) if column + 1 < ITERS else (devices, 8, 128)
        found, fresh, tile, *ends = apply_both(
            vectors, arrived, coef, tiles, SHIFTS[column], shape
        )
        tiles = (tile,)
        founds.append(found)
        vectors.append(fresh)
        if column + 1 < ITERS:
            arrived = exchange(*ends)
    parts = lax.all_to_all(tile, AXES, 0, 0)
    whole = pl.BlockSpec(memory_space=pltpu.VMEM)
    basis, search, small, least = pl.pallas_call(
        combine_kernel,
        name="combine",
        in_specs=[whole] * 8,
        out_specs=[whole] * 3 + [pl.BlockSpec(memory_space=pltpu.SMEM)],
        out_shape=[
            jax.ShapeDtypeStruct((ITERS + 1,) + start.shape, jnp.float32),
            jax.ShapeDtypeStruct((ITERS,) + start.shape, jnp.float32),
            jax.ShapeDtypeStruct((ITERS + 1, ITERS), jnp.float32),
            jax.ShapeDtypeStruct((1,), jnp.float32),
        ],
        compiler_params=pltpu.CompilerParams(vmem_limit_bytes=56 * 1024 * 1024),
    )(parts, *vectors, *founds)

    def body(state):
        begin = jnp.where(state[3][0] > 2.0, 0.0, start)
        basis, search, hess = step_by_step(begin, coef)
        return basis, search, hess, jnp.ones((1,), jnp.float32)

    basis, search, small, _ = lax.while_loop(
        lambda state: jnp.logical_not(state[3][0] >= PIVOT_FLOOR),
        body,
        (basis, search, small, least),
    )
    return basis, search, small


def solution(mesh):
    return jax.shard_map(
        per_device,
        mesh=mesh,
        in_specs=(
            P(None, "slab", "sub", None),
            P(None, "slab", "sub", None),
            P("slab", "sub", None),
            P("slab", "sub", None),
        ),
        out_specs=(P(None, None, "slab", "sub", None), P(None, None, "slab", "sub", None), P()),
        check_vma=False,
    )
```

```python
import functools

import jax
import jax.numpy as jnp
from jax import lax
from jax.experimental import pallas as pl
from jax.experimental.pallas import tpu as pltpu
from jax.sharding import PartitionSpec as P

ITERS = 3
AXES = ("slab", "sub")
SHIFTS = (1.5, 5.0, 4.5)
PIVOT_FLOOR = 0.01
PAD = 8


def neighbours(devices):
    up = [(i, i + 1) for i in range(devices - 1)]
    return up, [(j, i) for i, j in up]


def edge_rows(field, axis):
    sub = lax.axis_index("sub")
    start = (1 - sub) * (field.shape[axis] - PAD)
    return lax.dynamic_slice_in_dim(field, start, PAD, axis)


def across(field):
    return lax.ppermute(field, "sub", [(0, 1), (1, 0)])


def swap_pairs(devices, odd):
    mates = [(i, (i ^ 1) if not odd else (i + 1 if i % 2 else i - 1)) for i in range(devices)]
    return [(i, j) for i, j in mates if 0 <= j < devices]


def is_even():
    return lax.axis_index("slab") % 2 == 0


def split_ends(vector):
    length = vector.shape[1]
    last = [vector[3, length - 5 :]] + [vector[c, length - 2 :] for c in range(3)]
    first = [vector[3, :5]] + [vector[c, :2] for c in range(3)]
    return first, last


def for_pairs(first, last):
    even = is_even()
    first, last = jnp.concatenate(first, 0), jnp.concatenate(last, 0)
    return jnp.where(even, last, first), jnp.where(even, first, last)


def swap(to_near, to_far):
    devices = lax.axis_size("slab")
    near = lax.ppermute(to_near, "slab", swap_pairs(devices, False))
    far = lax.ppermute(to_far, "slab", swap_pairs(devices, True))
    corner = across(edge_rows(jnp.concatenate([near, far], 0), 1))
    return near, far, corner


def exchange_first(vector, stacked):
    names, length = stacked.shape[:2]
    flat = (names * 3,) + stacked.shape[2:]
    first, last = split_ends(vector)
    to_near, to_far = for_pairs(
        [stacked[:, :3].reshape(flat)] + first, [stacked[:, length - 3 :].reshape(flat)] + last
    )
    side_all = across(
        edge_rows(jnp.concatenate([vector.reshape((-1,) + vector.shape[2:]),
                                   stacked.reshape((-1,) + stacked.shape[2:])], 0), 1)
    )
    near, far, corner = swap(to_near, to_far)
    even, sub = is_even(), lax.axis_index("sub")
    planes, cut = near.shape[0], names * 3
    edge = (PAD,) + stacked.shape[3:]
    count = vector.shape[0] * length
    side = side_all[:count].reshape((vector.shape[0], length) + edge)
    low = jnp.where(even, far[:cut], near[:cut]).reshape((names, 3) + stacked.shape[2:])
    high = jnp.where(even, near[:cut], far[:cut]).reshape((names, 3) + stacked.shape[2:])
    from_near, from_far = corner[:cut], corner[planes : planes + cut]
    other = jnp.concatenate(
        [
            jnp.where(even, from_far, from_near).reshape((names, 3) + edge),
            side_all[count:].reshape((names, length) + edge),
            jnp.where(even, from_near, from_far).reshape((names, 3) + edge),
        ],
        1,
    )
    left = jnp.where(sub == 1, other, 0.0)
    right = jnp.where(sub == 0, other, 0.0)
    coef = jnp.concatenate([left, jnp.concatenate([low, stacked, high], 1), right], 2)
    return (near, far, side, corner), coef


def exchange(to_near, to_far, side_out):
    side = across(side_out)
    near, far, corner = swap(to_near, to_far)
    return near, far, side, corner


def plane_shifts(center):
    rows, lanes = center.shape
    lane = lax.broadcasted_iota(jnp.int32, center.shape, 1)
    y_plus = pltpu.roll(center, rows - 1, 0)
    y_minus = pltpu.roll(center, 1, 0)
    z_plus = jnp.where(lane == lanes - 1, 0.0, pltpu.roll(center, lanes - 1, 1))
    z_minus = jnp.where(lane == 0, 0.0, pltpu.roll(center, 1, 1))
    return y_plus, y_minus, z_plus, z_minus


def apply_kernel(
    count, shift, slabs, subs, skip, *refs
):
    place, near, far, side, corner, coef = refs[:6]
    olds = refs[6 : 6 + count]
    tiles = refs[6 + count : -12]
    found, new, tile_out, to_near, to_far, side_out = refs[-12:-6]
    pres, tee, schur, vel, first, second = refs[-6:]
    own = olds[-1]
    cells_x, cells_y, lanes = own.shape[1:]
    rows = cells_y + 2 * PAD
    slab, sub = place[0], place[1]
    is_left = sub == 0
    even = slab % 2 == 0

    def low(i):
        i, j = skip + i, near.shape[0] + skip + i
        return jnp.where(even, far[i], near[i]), jnp.where(even, corner[j], corner[i])

    def high(i):
        i, j = skip + i, near.shape[0] + skip + i
        return jnp.where(even, near[i], far[i]), jnp.where(even, corner[i], corner[j])

    def put(write, middle, beyond):
        write(slice(PAD, PAD + cells_y), middle)
        write(slice(0, PAD), jnp.where(is_left, 0.0, beyond))
        write(slice(PAD + cells_y, rows), jnp.where(is_left, beyond, 0.0))

    def writer(ref, *lead):
        def write(span, value):
            ref[(*lead, span, slice(None))] = value

        return write

    for i in range(5):
        put(writer(pres, i), *low(i))
        put(writer(pres, 5 + cells_x + i), *high(i))
    for c in range(3):
        for i in range(2):
            k = 5 + 2 * c + i
            put(writer(vel, c, i), *low(k))
            put(writer(vel, c, 2 + cells_x + i), *high(k))

    @pl.loop(0, cells_x)
    def _(i):
        put(writer(pres, 5 + i), own[3, i], side[3, i])
        for c in range(3):
            put(writer(vel, c, 2 + i), own[c, i], side[c, i])

    row = lax.broadcasted_iota(jnp.int32, (rows, lanes), 0) + (sub * cells_y - PAD)
    inside_y = (row >= 0) & (row < cells_y * subs)

    def inside(i, width):
        x = slab * cells_x - width + i
        good = ((x >= 0) & (x < cells_x * slabs)).astype(jnp.int32)
        return inside_y & (jnp.full((rows, lanes), good, jnp.int32) > 0)

    def transport(center, x_plus, x_minus, shifts, k):
        y_plus, y_minus, z_plus, z_minus = shifts
        total = x_plus + x_minus + y_plus + y_minus + z_plus + z_minus
        convect = coef[0, k] * (x_plus - x_minus) + coef[1, k] * (y_plus - y_minus)
        convect = convect + coef[2, k] * (z_plus - z_minus)
        return (6.0 + coef[3, k]) * center - total + 0.5 * convect

    @pl.loop(0, cells_x + 8, unroll=2 - cells_x % 2)
    def _(i):
        center = pres[i + 1]
        y_plus, y_minus, z_plus, z_minus = plane_shifts(center)
        total = pres[i + 2] + pres[i] + y_plus + y_minus + z_plus + z_minus
        tee[i] = jnp.where(inside(i, 4), center * (1.0 / 7.0) + total * (1.0 / 49.0), 0.0)

    @pl.loop(0, cells_x + 6, unroll=2 - cells_x % 2)
    def _(i):
        center = tee[i + 1]
        value = transport(center, tee[i + 2], tee[i], plane_shifts(center), i)
        schur[i] = jnp.where(inside(i, 3), -value / coef[4, i], 0.0)

    @pl.loop(0, cells_x + 4, unroll=2 - cells_x % 2)
    def _(i):
        center = schur[i + 1]
        y_plus, y_minus, z_plus, z_minus = plane_shifts(center)
        inverse = jnp.where(inside(i, 2), 1.0 / (6.0 + coef[3, i + 1]), 0.0)
        slopes = (schur[i + 2] - schur[i], y_plus - y_minus, z_plus - z_minus)
        for c in range(3):
            residue = vel[c, i] - 0.5 * slopes[c]
            vel[c, i] = residue
            first[c, i] = residue * inverse

    @pl.loop(0, cells_x + 2)
    def _(i):
        inverse = jnp.where(inside(i, 1), 1.0 / (6.0 + coef[3, i + 2]), 0.0)
        for c in range(3):
            center = first[c, i + 1]
            value = transport(
                center, first[c, i + 2], first[c, i], plane_shifts(center), i + 2
            )
            second[c, i] = center + (vel[c, i + 1] - value) * inverse

    mid = slice(PAD, PAD + cells_y)
    zero = jnp.zeros((cells_y, lanes), jnp.float32)

    def last_stage(i, sums):
        q = schur[i + 3]
        q_up, q_down = schur[i + 4], schur[i + 2]
        qy_plus, qy_minus, qz_plus, qz_minus = plane_shifts(q)
        slopes = (q_up - q_down, qy_plus - qy_minus, qz_plus - qz_minus)
        total = q_up + q_down + qy_plus + qy_minus + qz_plus + qz_minus
        div = jnp.zeros_like(q)
        images = []
        for c in range(3):
            center = second[c, i + 1]
            above, below = second[c, i + 2], second[c, i]
            shifts = plane_shifts(center)
            div = div + (above - below, shifts[0] - shifts[1], shifts[2] - shifts[3])[c]
            value = transport(center, above, below, shifts, i + 3)
            images.append(value + 0.5 * slopes[c])
            found[c, i] = center[mid]
        found[3, i] = q[mid]
        images.append(-0.5 * div - 0.5 * (6.0 * q - total))
        sums = list(sums)
        for c in range(4):
            fresh = images[c][mid] - shift * own[c, i]
            new[c, i] = fresh
            side_out[c, i] = jnp.where(is_left, fresh[cells_y - PAD :], fresh[:PAD])
            for k in range(count):
                sums[k] = sums[k] + fresh * olds[k][c, i]
            sums[count] = sums[count] + fresh * fresh
            if count == 1:
                old = own[c, i]
                sums[2] = sums[2] + old * old
        return tuple(sums)

    sums = lax.fori_loop(
        0, cells_x, last_stage, (zero,) * (count + 1 + (count == 1))
    )
    ends = [(3, i, cells_x - 5 + i) for i in range(5)]
    ends += [(c, i, cells_x - 2 + i) for c in range(3) for i in range(2)]
    for k, (c, i, j) in enumerate(ends):
        to_near[k] = jnp.where(even, new[c, j], new[c, i])
        to_far[k] = jnp.where(even, new[c, i], new[c, j])
    lane = lax.broadcasted_iota(jnp.int32, (8, 128), 1)
    base = count * (count + 1) // 2
    tile = tiles[0][...] if tiles else jnp.zeros((8, 128), jnp.float32)
    for k in range(count + 1):
        tile = jnp.where(lane == base + k, jnp.sum(sums[k]), tile)
    if count == 1:
        tile = jnp.where(lane == 0, jnp.sum(sums[2]), tile)
    tile_out[...] = jnp.broadcast_to(tile, tile_out.shape)


def apply_both(olds, arrived, coef, tiles, shift, tile_shape=(8, 128)):
    own = olds[-1]
    cells_x, cells_y, lanes = own.shape[1:]
    rows = cells_y + 2 * PAD
    place = jnp.stack([lax.axis_index("slab"), lax.axis_index("sub")]).astype(jnp.int32)
    whole = pl.BlockSpec(memory_space=pltpu.VMEM)
    f32 = jnp.float32
    return pl.pallas_call(
        functools.partial(
            apply_kernel, len(olds), shift, lax.axis_size("slab"), lax.axis_size("sub"),
            arrived[0].shape[0] - 11,
        ),
        name=f"apply_{len(olds)}",
        in_specs=[pl.BlockSpec(memory_space=pltpu.SMEM)] + [whole] * (5 + len(olds) + len(tiles)),
        out_specs=[whole] * 6,
        out_shape=[
            jax.ShapeDtypeStruct(own.shape, f32),
            jax.ShapeDtypeStruct(own.shape, f32),
            jax.ShapeDtypeStruct(tile_shape, f32),
            jax.ShapeDtypeStruct((11, cells_y, lanes), f32),
            jax.ShapeDtypeStruct((11, cells_y, lanes), f32),
            jax.ShapeDtypeStruct((4, cells_x, PAD, lanes), f32),
        ],
        scratch_shapes=[
            pltpu.VMEM((cells_x + 10, rows, lanes), f32),
            pltpu.VMEM((cells_x + 8, rows, lanes), f32),
            pltpu.VMEM((cells_x + 6, rows, lanes), f32),
            pltpu.VMEM((3, cells_x + 4, rows, lanes), f32),
            pltpu.VMEM((3, cells_x + 4, rows, lanes), f32),
            pltpu.VMEM((3, cells_x + 2, rows, lanes), f32),
        ],
        compiler_params=pltpu.CompilerParams(vmem_limit_bytes=56 * 1024 * 1024),
    )(place, *arrived, coef, *olds, *tiles)


def combine_kernel(*refs):
    parts = refs[0]
    vectors, founds = refs[1:5], refs[5:8]
    basis, search, small, least = refs[8:]
    total = jnp.sum(parts[...], axis=0)[0:1]
    lane = lax.broadcasted_iota(jnp.int32, (1, 128), 1)

    def gram(a, b):
        a, b = max(a, b), min(a, b)
        at = a * (a + 1) // 2 + b
        return jnp.sum(jnp.where(lane == at, total, 0.0), axis=1, keepdims=True)

    n = ITERS + 1
    upper, share = {}, None
    for j in range(n):
        for i in range(j):
            value = gram(i, j)
            for k in range(i):
                value = value - upper[k, i] * upper[k, j]
            upper[i, j] = value / upper[i, i]
        full = gram(j, j)
        left = full
        for k in range(j):
            left = left - upper[k, j] * upper[k, j]
        share = left / full if share is None else jnp.minimum(share, left / full)
        upper[j, j] = jnp.sqrt(left)
    inverse = {}
    for j in range(n):
        inverse[j, j] = 1.0 / upper[j, j]
        for i in range(j - 1, -1, -1):
            value = upper[i, i + 1] * inverse[i + 1, j]
            for k in range(i + 2, j + 1):
                value = value + upper[i, k] * inverse[k, j]
            inverse[i, j] = -value / upper[i, i]
    rows = lax.broadcasted_iota(jnp.int32, (8, 128), 0)
    lanes = lax.broadcasted_iota(jnp.int32, (8, 128), 1)
    tile = jnp.zeros((8, 128), jnp.float32)
    for j in range(ITERS):
        for i in range(j + 2):
            value = None
            for k in range(max(i - 1, 0), j + 1):
                moved = upper[i, k + 1]
                if i <= k:
                    moved = moved + SHIFTS[k] * upper[i, k]
                term = moved * inverse[k, j]
                value = term if value is None else value + term
            tile = jnp.where((rows == i) & (lanes == j), value, tile)
    small[...] = tile[: ITERS + 1, :ITERS]
    least[0] = jnp.sum(share)

    @pl.loop(0, vectors[0].shape[1])
    def _(x):
        for c in range(4):
            for count, sources, target in ((n, vectors, basis), (ITERS, founds, search)):
                planes = [source[c, x] for source in sources]
                for j in range(count):
                    value = planes[0] * inverse[0, j]
                    for i in range(1, j + 1):
                        value = value + planes[i] * inverse[i, j]
                    target[j, c, x] = value


def step_by_step(start, coef):
    def total(value):
        return lax.psum(jnp.sum(value), AXES)

    vectors = [start / jnp.sqrt(total(start * start))]
    searches = []
    hess = jnp.zeros((ITERS + 1, ITERS), jnp.float32)
    for column in range(ITERS):
        own = vectors[column]
        arrived = exchange(*for_pairs(*split_ends(own)), edge_rows(own, 2))
        found, image = apply_both([own], arrived, coef, (), 0.0)[:2]
        searches.append(found)
        projected = [total(vector * image) for vector in vectors]
        for row in range(column + 1):
            image = image - projected[row] * vectors[row]
            hess = hess.at[row, column].set(projected[row])
        norm_next = jnp.sqrt(total(image * image))
        hess = hess.at[column + 1, column].set(norm_next)
        vectors.append(image / norm_next)
    return jnp.stack(vectors), jnp.stack(searches), hess


def per_device(start, wind, reaction, mass):
    arrived, coef = exchange_first(start, jnp.concatenate([wind, reaction[None], mass[None]], 0))
    devices = lax.axis_size("slab") * lax.axis_size("sub")
    tiles = ()
    vectors, founds = [start], []
    for column in range(ITERS):
        shape = (8, 128) if column + 1 < ITERS else (devices, 8, 128)
        found, fresh, tile, *ends = apply_both(
            vectors, arrived, coef, tiles, SHIFTS[column], shape
        )
        tiles = (tile,)
        founds.append(found)
        vectors.append(fresh)
        if column + 1 < ITERS:
            arrived = exchange(*ends)
    parts = lax.all_to_all(tile, AXES, 0, 0)
    whole = pl.BlockSpec(memory_space=pltpu.VMEM)
    basis, search, small, least = pl.pallas_call(
        combine_kernel,
        name="combine",
        in_specs=[whole] * 8,
        out_specs=[whole] * 3 + [pl.BlockSpec(memory_space=pltpu.SMEM)],
        out_shape=[
            jax.ShapeDtypeStruct((ITERS + 1,) + start.shape, jnp.float32),
            jax.ShapeDtypeStruct((ITERS,) + start.shape, jnp.float32),
            jax.ShapeDtypeStruct((ITERS + 1, ITERS), jnp.float32),
            jax.ShapeDtypeStruct((1,), jnp.float32),
        ],
        compiler_params=pltpu.CompilerParams(vmem_limit_bytes=56 * 1024 * 1024),
    )(parts, *vectors, *founds)

    def body(state):
        begin = jnp.where(state[3][0] > 2.0, 0.0, start)
        basis, search, hess = step_by_step(begin, coef)
        return basis, search, hess, jnp.ones((1,), jnp.float32)

    basis, search, small, _ = lax.while_loop(
        lambda state: jnp.logical_not(state[3][0] >= PIVOT_FLOOR),
        body,
        (basis, search, small, least),
    )
    return basis, search, small


def solution(mesh):
    return jax.shard_map(
        per_device,
        mesh=mesh,
        in_specs=(
            P(None, "slab", "sub", None),
            P(None, "slab", "sub", None),
            P("slab", "sub", None),
            P("slab", "sub", None),
        ),
        out_specs=(P(None, None, "slab", "sub", None), P(None, None, "slab", "sub", None), P()),
        check_vma=False,
    )
```

```python
import functools

import jax
import jax.numpy as jnp
from jax import lax
from jax.experimental import pallas as pl
from jax.experimental.pallas import tpu as pltpu
from jax.sharding import PartitionSpec as P

ITERS = 3
AXES = ("slab", "sub")
SHIFTS = (1.5, 5.0, 4.5)
PIVOT_FLOOR = 0.01
PAD = 8


def neighbours(devices):
    up = [(i, i + 1) for i in range(devices - 1)]
    return up, [(j, i) for i, j in up]


def edge_rows(field, axis):
    sub = lax.axis_index("sub")
    start = (1 - sub) * (field.shape[axis] - PAD)
    return lax.dynamic_slice_in_dim(field, start, PAD, axis)


def across(field):
    return lax.ppermute(field, "sub", [(0, 1), (1, 0)])


def swap_pairs(devices, odd):
    mates = [(i, (i ^ 1) if not odd else (i + 1 if i % 2 else i - 1)) for i in range(devices)]
    return [(i, j) for i, j in mates if 0 <= j < devices]


def is_even():
    return lax.axis_index("slab") % 2 == 0


def split_ends(vector):
    length = vector.shape[1]
    last = [vector[3, length - 5 :]] + [vector[c, length - 2 :] for c in range(3)]
    first = [vector[3, :5]] + [vector[c, :2] for c in range(3)]
    return first, last


def for_pairs(first, last):
    even = is_even()
    first, last = jnp.concatenate(first, 0), jnp.concatenate(last, 0)
    return jnp.where(even, last, first), jnp.where(even, first, last)


def swap(to_near, to_far):
    devices = lax.axis_size("slab")
    near = lax.ppermute(to_near, "slab", swap_pairs(devices, False))
    far = lax.ppermute(to_far, "slab", swap_pairs(devices, True))
    corner = across(edge_rows(jnp.concatenate([near, far], 0), 1))
    return near, far, corner


def exchange_first(vector, stacked):
    names, length = stacked.shape[:2]
    flat = (names * 3,) + stacked.shape[2:]
    first, last = split_ends(vector)
    to_near, to_far = for_pairs(
        [stacked[:, :3].reshape(flat)] + first, [stacked[:, length - 3 :].reshape(flat)] + last
    )
    side_all = across(
        edge_rows(jnp.concatenate([vector.reshape((-1,) + vector.shape[2:]),
                                   stacked.reshape((-1,) + stacked.shape[2:])], 0), 1)
    )
    near, far, corner = swap(to_near, to_far)
    even, sub = is_even(), lax.axis_index("sub")
    planes, cut = near.shape[0], names * 3
    edge = (PAD,) + stacked.shape[3:]
    count = vector.shape[0] * length
    side = side_all[:count].reshape((vector.shape[0], length) + edge)
    low = jnp.where(even, far[:cut], near[:cut]).reshape((names, 3) + stacked.shape[2:])
    high = jnp.where(even, near[:cut], far[:cut]).reshape((names, 3) + stacked.shape[2:])
    from_near, from_far = corner[:cut], corner[planes : planes + cut]
    other = jnp.concatenate(
        [
            jnp.where(even, from_far, from_near).reshape((names, 3) + edge),
            side_all[count:].reshape((names, length) + edge),
            jnp.where(even, from_near, from_far).reshape((names, 3) + edge),
        ],
        1,
    )
    left = jnp.where(sub == 1, other, 0.0)
    right = jnp.where(sub == 0, other, 0.0)
    coef = jnp.concatenate([left, jnp.concatenate([low, stacked, high], 1), right], 2)
    return (near, far, side, corner), coef


def exchange(to_near, to_far, side_out):
    side = across(side_out)
    near, far, corner = swap(to_near, to_far)
    return near, far, side, corner


def plane_shifts(center):
    rows, lanes = center.shape
    lane = lax.broadcasted_iota(jnp.int32, center.shape, 1)
    y_plus = pltpu.roll(center, rows - 1, 0)
    y_minus = pltpu.roll(center, 1, 0)
    z_plus = jnp.where(lane == lanes - 1, 0.0, pltpu.roll(center, lanes - 1, 1))
    z_minus = jnp.where(lane == 0, 0.0, pltpu.roll(center, 1, 1))
    return y_plus, y_minus, z_plus, z_minus


def apply_kernel(
    count, shift, slabs, subs, skip, *refs
):
    place, near, far, side, corner, coef = refs[:6]
    olds = refs[6 : 6 + count]
    tiles = refs[6 + count : -12]
    found, new, tile_out, to_near, to_far, side_out = refs[-12:-6]
    pres, tee, schur, vel, first, second = refs[-6:]
    own = olds[-1]
    cells_x, cells_y, lanes = own.shape[1:]
    rows = cells_y + 2 * PAD
    slab, sub = place[0], place[1]
    is_left = sub == 0
    even = slab % 2 == 0

    def low(i):
        i, j = skip + i, near.shape[0] + skip + i
        return jnp.where(even, far[i], near[i]), jnp.where(even, corner[j], corner[i])

    def high(i):
        i, j = skip + i, near.shape[0] + skip + i
        return jnp.where(even, near[i], far[i]), jnp.where(even, corner[i], corner[j])

    def put(write, middle, beyond):
        write(slice(PAD, PAD + cells_y), middle)
        write(slice(0, PAD), jnp.where(is_left, 0.0, beyond))
        write(slice(PAD + cells_y, rows), jnp.where(is_left, beyond, 0.0))

    def writer(ref, *lead):
        def write(span, value):
            ref[(*lead, span, slice(None))] = value

        return write

    for i in range(5):
        put(writer(pres, i), *low(i))
        put(writer(pres, 5 + cells_x + i), *high(i))
    for c in range(3):
        for i in range(2):
            k = 5 + 2 * c + i
            put(writer(vel, c, i), *low(k))
            put(writer(vel, c, 2 + cells_x + i), *high(k))

    @pl.loop(0, cells_x, unroll=2 - cells_x % 2)
    def _(i):
        put(writer(pres, 5 + i), own[3, i], side[3, i])
        for c in range(3):
            put(writer(vel, c, 2 + i), own[c, i], side[c, i])

    row = lax.broadcasted_iota(jnp.int32, (rows, lanes), 0) + (sub * cells_y - PAD)
    inside_y = (row >= 0) & (row < cells_y * subs)

    def inside(i, width):
        x = slab * cells_x - width + i
        good = ((x >= 0) & (x < cells_x * slabs)).astype(jnp.int32)
        return inside_y & (jnp.full((rows, lanes), good, jnp.int32) > 0)

    def transport(center, x_plus, x_minus, shifts, k):
        y_plus, y_minus, z_plus, z_minus = shifts
        total = x_plus + x_minus + y_plus + y_minus + z_plus + z_minus
        convect = coef[0, k] * (x_plus - x_minus) + coef[1, k] * (y_plus - y_minus)
        convect = convect + coef[2, k] * (z_plus - z_minus)
        return (6.0 + coef[3, k]) * center - total + 0.5 * convect

    @pl.loop(0, cells_x + 8, unroll=2 - cells_x % 2)
    def _(i):
        center = pres[i + 1]
        y_plus, y_minus, z_plus, z_minus = plane_shifts(center)
        total = pres[i + 2] + pres[i] + y_plus + y_minus + z_plus + z_minus
        tee[i] = jnp.where(inside(i, 4), center * (1.0 / 7.0) + total * (1.0 / 49.0), 0.0)

    @pl.loop(0, cells_x + 6, unroll=2 - cells_x % 2)
    def _(i):
        center = tee[i + 1]
        value = transport(center, tee[i + 2], tee[i], plane_shifts(center), i)
        schur[i] = jnp.where(inside(i, 3), -value / coef[4, i], 0.0)

    @pl.loop(0, cells_x + 4, unroll=2 - cells_x % 2)
    def _(i):
        center = schur[i + 1]
        y_plus, y_minus, z_plus, z_minus = plane_shifts(center)
        inverse = jnp.where(inside(i, 2), 1.0 / (6.0 + coef[3, i + 1]), 0.0)
        slopes = (schur[i + 2] - schur[i], y_plus - y_minus, z_plus - z_minus)
        for c in range(3):
            residue = vel[c, i] - 0.5 * slopes[c]
            vel[c, i] = residue
            first[c, i] = residue * inverse

    @pl.loop(0, cells_x + 2, unroll=2 - cells_x % 2)
    def _(i):
        inverse = jnp.where(inside(i, 1), 1.0 / (6.0 + coef[3, i + 2]), 0.0)
        for c in range(3):
            center = first[c, i + 1]
            value = transport(
                center, first[c, i + 2], first[c, i], plane_shifts(center), i + 2
            )
            second[c, i] = center + (vel[c, i + 1] - value) * inverse

    mid = slice(PAD, PAD + cells_y)
    zero = jnp.zeros((cells_y, lanes), jnp.float32)

    def last_stage(i, sums):
        q = schur[i + 3]
        q_up, q_down = schur[i + 4], schur[i + 2]
        qy_plus, qy_minus, qz_plus, qz_minus = plane_shifts(q)
        slopes = (q_up - q_down, qy_plus - qy_minus, qz_plus - qz_minus)
        total = q_up + q_down + qy_plus + qy_minus + qz_plus + qz_minus
        div = jnp.zeros_like(q)
        images = []
        for c in range(3):
            center = second[c, i + 1]
            above, below = second[c, i + 2], second[c, i]
            shifts = plane_shifts(center)
            div = div + (above - below, shifts[0] - shifts[1], shifts[2] - shifts[3])[c]
            value = transport(center, above, below, shifts, i + 3)
            images.append(value + 0.5 * slopes[c])
            found[c, i] = center[mid]
        found[3, i] = q[mid]
        images.append(-0.5 * div - 0.5 * (6.0 * q - total))
        sums = list(sums)
        for c in range(4):
            fresh = images[c][mid] - shift * own[c, i]
            new[c, i] = fresh
            side_out[c, i] = jnp.where(is_left, fresh[cells_y - PAD :], fresh[:PAD])
            for k in range(count):
                sums[k] = sums[k] + fresh * olds[k][c, i]
            sums[count] = sums[count] + fresh * fresh
            if count == 1:
                old = own[c, i]
                sums[2] = sums[2] + old * old
        return tuple(sums)

    sums = lax.fori_loop(
        0, cells_x, last_stage, (zero,) * (count + 1 + (count == 1))
    )
    ends = [(3, i, cells_x - 5 + i) for i in range(5)]
    ends += [(c, i, cells_x - 2 + i) for c in range(3) for i in range(2)]
    for k, (c, i, j) in enumerate(ends):
        to_near[k] = jnp.where(even, new[c, j], new[c, i])
        to_far[k] = jnp.where(even, new[c, i], new[c, j])
    lane = lax.broadcasted_iota(jnp.int32, (8, 128), 1)
    base = count * (count + 1) // 2
    tile = tiles[0][...] if tiles else jnp.zeros((8, 128), jnp.float32)
    for k in range(count + 1):
        tile = jnp.where(lane == base + k, jnp.sum(sums[k]), tile)
    if count == 1:
        tile = jnp.where(lane == 0, jnp.sum(sums[2]), tile)
    tile_out[...] = jnp.broadcast_to(tile, tile_out.shape)


def apply_both(olds, arrived, coef, tiles, shift, tile_shape=(8, 128)):
    own = olds[-1]
    cells_x, cells_y, lanes = own.shape[1:]
    rows = cells_y + 2 * PAD
    place = jnp.stack([lax.axis_index("slab"), lax.axis_index("sub")]).astype(jnp.int32)
    whole = pl.BlockSpec(memory_space=pltpu.VMEM)
    f32 = jnp.float32
    return pl.pallas_call(
        functools.partial(
            apply_kernel, len(olds), shift, lax.axis_size("slab"), lax.axis_size("sub"),
            arrived[0].shape[0] - 11,
        ),
        name=f"apply_{len(olds)}",
        in_specs=[pl.BlockSpec(memory_space=pltpu.SMEM)] + [whole] * (5 + len(olds) + len(tiles)),
        out_specs=[whole] * 6,
        out_shape=[
            jax.ShapeDtypeStruct(own.shape, f32),
            jax.ShapeDtypeStruct(own.shape, f32),
            jax.ShapeDtypeStruct(tile_shape, f32),
            jax.ShapeDtypeStruct((11, cells_y, lanes), f32),
            jax.ShapeDtypeStruct((11, cells_y, lanes), f32),
            jax.ShapeDtypeStruct((4, cells_x, PAD, lanes), f32),
        ],
        scratch_shapes=[
            pltpu.VMEM((cells_x + 10, rows, lanes), f32),
            pltpu.VMEM((cells_x + 8, rows, lanes), f32),
            pltpu.VMEM((cells_x + 6, rows, lanes), f32),
            pltpu.VMEM((3, cells_x + 4, rows, lanes), f32),
            pltpu.VMEM((3, cells_x + 4, rows, lanes), f32),
            pltpu.VMEM((3, cells_x + 2, rows, lanes), f32),
        ],
        compiler_params=pltpu.CompilerParams(vmem_limit_bytes=56 * 1024 * 1024),
    )(place, *arrived, coef, *olds, *tiles)


def combine_kernel(*refs):
    parts = refs[0]
    vectors, founds = refs[1:5], refs[5:8]
    basis, search, small, least = refs[8:]
    total = jnp.sum(parts[...], axis=0)[0:1]
    lane = lax.broadcasted_iota(jnp.int32, (1, 128), 1)

    def gram(a, b):
        a, b = max(a, b), min(a, b)
        at = a * (a + 1) // 2 + b
        return jnp.sum(jnp.where(lane == at, total, 0.0), axis=1, keepdims=True)

    n = ITERS + 1
    upper, share = {}, None
    for j in range(n):
        for i in range(j):
            value = gram(i, j)
            for k in range(i):
                value = value - upper[k, i] * upper[k, j]
            upper[i, j] = value / upper[i, i]
        full = gram(j, j)
        left = full
        for k in range(j):
            left = left - upper[k, j] * upper[k, j]
        share = left / full if share is None else jnp.minimum(share, left / full)
        upper[j, j] = jnp.sqrt(left)
    inverse = {}
    for j in range(n):
        inverse[j, j] = 1.0 / upper[j, j]
        for i in range(j - 1, -1, -1):
            value = upper[i, i + 1] * inverse[i + 1, j]
            for k in range(i + 2, j + 1):
                value = value + upper[i, k] * inverse[k, j]
            inverse[i, j] = -value / upper[i, i]
    rows = lax.broadcasted_iota(jnp.int32, (8, 128), 0)
    lanes = lax.broadcasted_iota(jnp.int32, (8, 128), 1)
    tile = jnp.zeros((8, 128), jnp.float32)
    for j in range(ITERS):
        for i in range(j + 2):
            value = None
            for k in range(max(i - 1, 0), j + 1):
                moved = upper[i, k + 1]
                if i <= k:
                    moved = moved + SHIFTS[k] * upper[i, k]
                term = moved * inverse[k, j]
                value = term if value is None else value + term
            tile = jnp.where((rows == i) & (lanes == j), value, tile)
    small[...] = tile[: ITERS + 1, :ITERS]
    least[0] = jnp.sum(share)

    @pl.loop(0, vectors[0].shape[1])
    def _(x):
        for c in range(4):
            for count, sources, target in ((n, vectors, basis), (ITERS, founds, search)):
                planes = [source[c, x] for source in sources]
                for j in range(count):
                    value = planes[0] * inverse[0, j]
                    for i in range(1, j + 1):
                        value = value + planes[i] * inverse[i, j]
                    target[j, c, x] = value


def step_by_step(start, coef):
    def total(value):
        return lax.psum(jnp.sum(value), AXES)

    vectors = [start / jnp.sqrt(total(start * start))]
    searches = []
    hess = jnp.zeros((ITERS + 1, ITERS), jnp.float32)
    for column in range(ITERS):
        own = vectors[column]
        arrived = exchange(*for_pairs(*split_ends(own)), edge_rows(own, 2))
        found, image = apply_both([own], arrived, coef, (), 0.0)[:2]
        searches.append(found)
        projected = [total(vector * image) for vector in vectors]
        for row in range(column + 1):
            image = image - projected[row] * vectors[row]
            hess = hess.at[row, column].set(projected[row])
        norm_next = jnp.sqrt(total(image * image))
        hess = hess.at[column + 1, column].set(norm_next)
        vectors.append(image / norm_next)
    return jnp.stack(vectors), jnp.stack(searches), hess


def per_device(start, wind, reaction, mass):
    arrived, coef = exchange_first(start, jnp.concatenate([wind, reaction[None], mass[None]], 0))
    devices = lax.axis_size("slab") * lax.axis_size("sub")
    tiles = ()
    vectors, founds = [start], []
    for column in range(ITERS):
        shape = (8, 128) if column + 1 < ITERS else (devices, 8, 128)
        found, fresh, tile, *ends = apply_both(
            vectors, arrived, coef, tiles, SHIFTS[column], shape
        )
        tiles = (tile,)
        founds.append(found)
        vectors.append(fresh)
        if column + 1 < ITERS:
            arrived = exchange(*ends)
    parts = lax.all_to_all(tile, AXES, 0, 0)
    whole = pl.BlockSpec(memory_space=pltpu.VMEM)
    basis, search, small, least = pl.pallas_call(
        combine_kernel,
        name="combine",
        in_specs=[whole] * 8,
        out_specs=[whole] * 3 + [pl.BlockSpec(memory_space=pltpu.SMEM)],
        out_shape=[
            jax.ShapeDtypeStruct((ITERS + 1,) + start.shape, jnp.float32),
            jax.ShapeDtypeStruct((ITERS,) + start.shape, jnp.float32),
            jax.ShapeDtypeStruct((ITERS + 1, ITERS), jnp.float32),
            jax.ShapeDtypeStruct((1,), jnp.float32),
        ],
        compiler_params=pltpu.CompilerParams(vmem_limit_bytes=56 * 1024 * 1024),
    )(parts, *vectors, *founds)

    def body(state):
        begin = jnp.where(state[3][0] > 2.0, 0.0, start)
        basis, search, hess = step_by_step(begin, coef)
        return basis, search, hess, jnp.ones((1,), jnp.float32)

    basis, search, small, _ = lax.while_loop(
        lambda state: jnp.logical_not(state[3][0] >= PIVOT_FLOOR),
        body,
        (basis, search, small, least),
    )
    return basis, search, small


def solution(mesh):
    return jax.shard_map(
        per_device,
        mesh=mesh,
        in_specs=(
            P(None, "slab", "sub", None),
            P(None, "slab", "sub", None),
            P("slab", "sub", None),
            P("slab", "sub", None),
        ),
        out_specs=(P(None, None, "slab", "sub", None), P(None, None, "slab", "sub", None), P()),
        check_vma=False,
    )
```
